32 devices in a mesh: section: 4 (over x, core), dp: 8 (over z, y).
Axes of the slice: x: 2, y: 2, z: 4, core: 2. Of those that a mesh axis runs over, the one named last changes fastest.
Arguments:
- student_states: bfloat16 [64, 512, 1024], P('dp'), may hold values from -6 to 6
- lengths: int32 [64], P('dp'), may hold values from 64 to 512
- student_ln_gain: float32 [1024], replicated, may hold values from 0.1 to 1.9
- student_w_in: bfloat16 [1024, 4096], P(None, 'section'), may hold values from -0.1875 to 0.1875
- student_w_out: bfloat16 [4096, 1024], P('section'), may hold values from -0.09375 to 0.09375
- teacher_rows: bfloat16 [64, 4096], P('dp'), may hold values from -6 to 6
- teacher_mlp_gain: float32 [4096], replicated, may hold values from 0.1 to 1.9
- teacher_gate_up: bfloat16 [2, 4096, 12288], P(None, 'dp', 'section'), may hold values from -0.09375 to 0.09375
- teacher_down: bfloat16 [12288, 4096], P('section', 'dp'), may hold values from -0.0546875 to 0.0546875
- teacher_final_gain: float32 [4096], replicated, may hold values from 0.1 to 1.9
Outputs:
- loss: float32 [], replicated
- grad_w_in: float32 [1024, 4096], P('dp', 'section')
- grad_w_out: float32 [4096, 1024], P(('section', 'dp'))
- teacher_states: float32 [64, 4096], P('dp', 'section')
The draws below stay inside these ranges and needn't reach their ends.
Inputs may be any that keep to these rules, and one draw needn't show every extreme that they name: Each document's first lengths tokens are real, the rest padding.
All inputs are finite; a program needn't handle non-finite values.
Results may differ from the reference program's by a relative error of at most 0.013.
The reference program's roundings to bfloat16 on the way count: a program that leaves them out, or rounds other values in their place, can miss the bound.
Values may be sent and summed in bfloat16 or wider, within the bound.
No kernel may reach another device: no remote copies, remote signals or barrier semaphores. Data moves between devices by JAX's collectives and lax.ppermute only.
A program may use at most 128 MiB of HBM per device.

```python
import jax
import jax.numpy as jnp
from jax import lax

D_T = 4096
FF_T = 12288
D_S = 1024
FF_S = 4096
SEQ = 512
DOC_DEV = 8
DOCS = 64
N_DP = 8


def place_ends(entries, rng, smallest, high):
    longest = entries.shape.index(max(entries.shape))
    spots = []
    for shift in (0, 1):
        where = [jax.random.randint(jax.random.fold_in(rng, axis), (), 0, length) for axis, length in enumerate(entries.shape)]
        where[longest] = (where[longest] + shift) % entries.shape[longest]
        spots.append(tuple(where))
    return entries.at[spots[0]].set(smallest).at[spots[1]].set(high)


def spiked(drawn, own_key, source, target, shards_of, factor):
    owner, partner = [(jnp.arange(drawn.shape[axis_at]) // (drawn.shape[axis_at] // shards_of)).reshape([-1 if axis == axis_at else 1 for axis in range(drawn.ndim)]) for axis_at in (source, target)]
    chosen = jax.random.permutation(own_key, shards_of)[partner]
    strong = (owner == chosen) | (owner == (partner + shards_of // 2) % shards_of)
    return jnp.where(strong, factor * drawn, drawn)


def block_scale(stream_key, shape, cuts, smallest, high):
    def one(position, shards_of):
        steps = jax.random.uniform(jax.random.fold_in(jax.random.fold_in(stream_key, 6), position), (shards_of,), jnp.float32, smallest / len(cuts), high / len(cuts))
        return jnp.repeat(jnp.exp(steps), shape[position] // shards_of).reshape((-1,) + (1,) * (len(shape) - position - 1))

    level = one(*cuts[0])
    for cut in cuts[1:]:
        level = level * one(*cut)
    return level


def centred(rng, extent, width, bound, split=(), kind=jnp.bfloat16):
    result = width * jax.random.normal(rng, extent, jnp.float32)
    if split:
        result = result * block_scale(rng, extent, split, -0.22, 0.18)
    return jnp.clip(result, -bound, bound).astype(kind)


def heavy_noise(own_key, extent, deviation, reach, shards, heavy, kind=jnp.bfloat16):
    result = deviation * jax.random.normal(own_key, extent, jnp.float32)
    if shards:
        result = result * block_scale(own_key, extent, shards, -0.22, 0.18)
    return jnp.clip(spiked(result, jax.random.fold_in(own_key, 3), *heavy), -reach, reach).astype(kind)


def setup_inputs(seed: int = 0) -> dict:
    key_list = jax.random.split(jax.random.key(seed), 11)
    return {
        "student_states": heavy_noise(key_list[0], (DOCS, SEQ, D_S), 1.0, 6.0, ((0, 8),), (0, 2, 8, 2.0)),
        "lengths": place_ends(jax.random.randint(key_list[1], (DOCS,), SEQ // 8, SEQ + 1), jax.random.fold_in(key_list[1], 1), SEQ // 8, SEQ).astype(jnp.int32),
        "student_ln_gain": jnp.clip(1.0 + 0.18 * jax.random.normal(key_list[2], (D_S,), jnp.float32), 0.1, 1.9),
        "student_w_in": centred(key_list[3], (D_S, FF_S), D_S ** -0.5, 0.1875, ((1, 4),)),
        "student_w_out": centred(key_list[4], (FF_S, D_S), FF_S ** -0.5, 0.09375, ((0, 4),)),
        "teacher_rows": centred(key_list[5], (DOCS, D_T), 1.0, 6.0, ((0, 8),)),
        "teacher_mlp_gain": jnp.clip(1.0 + 0.18 * jax.random.normal(key_list[6], (D_T,), jnp.float32), 0.1, 1.9),
        "teacher_gate_up": centred(key_list[7], (2, D_T, FF_T), D_T ** -0.5, 0.09375, ((1, 8), (2, 4))),
        "teacher_down": centred(key_list[8], (FF_T, D_T), FF_T ** -0.5, 0.0546875, ((0, 4), (1, 8))),
        "teacher_final_gain": jnp.clip(1.0 + 0.18 * jax.random.normal(key_list[9], (D_T,), jnp.float32), 0.1, 1.9),
    }


student_softness = 0.05
teacher_softness = 0.02

def layer_norm(states, gain):
    values = states.astype(jnp.float32)
    center = values - lax.optimization_barrier(jnp.mean(values, -1, keepdims=True))
    spread = lax.optimization_barrier(jnp.mean(center * center, -1, keepdims=True))
    return (center * lax.rsqrt(spread + 1e-05) * gain).astype(jnp.bfloat16)

def gelu_exact(value):
    return 0.5 * value * (1.0 + jax.scipy.special.erf(value * 0.7071067811865476))

def gelu_slope(value):
    return 0.5 * (1.0 + jax.scipy.special.erf(value * 0.7071067811865476)) + value * jnp.exp(-0.5 * value * value) * 0.3989422804014327

def contrast(student_logits, teacher_logits, row_ids, col_ids):
    keep = row_ids[:, None] != col_ids[None, :]
    partner = (row_ids + 1 - 2 * (row_ids % 2))[:, None] == col_ids[None, :]
    s_exp = jnp.where(keep, jnp.exp(student_logits), 0.0)
    t_exp = jnp.where(keep, jnp.exp(teacher_logits), 0.0)
    s_total = lax.optimization_barrier(jnp.sum(s_exp, -1, keepdims=True))
    t_total = lax.optimization_barrier(jnp.sum(t_exp, -1, keepdims=True))
    s_prob = s_exp / s_total
    t_prob = t_exp / t_total
    s_log = student_logits - jnp.log(s_total)
    t_log = teacher_logits - jnp.log(t_total)
    terms = jnp.where(partner, -s_log, 0.0) + jnp.where(keep, t_prob * (t_log - s_log), 0.0)
    gradient_list = 2.0 * s_prob - partner.astype(jnp.float32) - t_prob
    return (gradient_list, jnp.sum(terms))

def reference(student_states, lengths, student_ln_gain, student_w_in, student_w_out, teacher_rows, teacher_mlp_gain, teacher_gate_up, teacher_down, teacher_final_gain):
    rows_f = teacher_rows.astype(jnp.float32)
    inverse = lax.rsqrt(lax.optimization_barrier(jnp.mean(rows_f * rows_f, -1, keepdims=True)) + 1e-06)
    normed = (rows_f * inverse * teacher_mlp_gain).astype(jnp.bfloat16)
    gate = jnp.dot(normed, teacher_gate_up[0], preferred_element_type=jnp.float32)
    upper = jnp.dot(normed, teacher_gate_up[1], preferred_element_type=jnp.float32)
    hidden = (jax.nn.silu(gate) * upper).astype(jnp.bfloat16)
    teacher_states = rows_f + jnp.dot(hidden, teacher_down, preferred_element_type=jnp.float32)
    scaled = teacher_states * teacher_final_gain
    teacher_normalized = scaled / jnp.sqrt(lax.optimization_barrier(jnp.sum(scaled * scaled, -1, keepdims=True)) + 1e-06)
    positions = jnp.arange(SEQ, dtype=jnp.int32)
    masks = (positions[None, :] < lengths[:, None]).astype(jnp.float32)
    counts = lengths.astype(jnp.float32)[:, None]
    state_blocks = student_states.reshape(N_DP, DOC_DEV, SEQ, D_S)
    mask_blocks = masks.reshape(N_DP, DOC_DEV, SEQ)

    def forward_block(pair):
        block, mask = pair
        tokens = layer_norm(block, student_ln_gain).reshape(DOC_DEV * SEQ, D_S)
        pre_act = jnp.dot(tokens, student_w_in, preferred_element_type=jnp.float32)
        act = gelu_exact(pre_act).astype(jnp.bfloat16)
        act = lax.optimization_barrier(act).astype(jnp.float32).reshape(DOC_DEV, SEQ, FF_S)
        pool_act = jnp.einsum('bs,bsf->bf', mask, act)
        pool_x = jnp.einsum('bs,bse->be', mask, block.astype(jnp.float32))
        return (pool_act, pool_x)
    pool_act, pool_x = lax.map(forward_block, (state_blocks, mask_blocks))
    pool_act = pool_act.reshape(DOCS, FF_S)
    pool_x = pool_x.reshape(DOCS, D_S)
    pooled_act = (pool_act / counts).astype(jnp.bfloat16)
    student_raw = pool_x / counts + jnp.dot(pooled_act, student_w_out, preferred_element_type=jnp.float32)
    norms = jnp.sqrt(lax.optimization_barrier(jnp.sum(student_raw * student_raw, -1, keepdims=True)) + 1e-06)
    student_normalized = student_raw / norms
    student_logits = jnp.dot(student_normalized, student_normalized.T, precision=lax.Precision.HIGHEST) / student_softness
    teacher_logits = jnp.dot(teacher_normalized, teacher_normalized.T, precision=lax.Precision.HIGHEST) / teacher_softness
    row_ids = jnp.arange(DOCS, dtype=jnp.int32)
    gradient_list, loss = contrast(student_logits, teacher_logits, row_ids, row_ids)
    normalized_gradient = jnp.dot(gradient_list + gradient_list.T, student_normalized, precision=lax.Precision.HIGHEST) / student_softness
    raw_grad = (normalized_gradient - student_normalized * lax.optimization_barrier(jnp.sum(student_normalized * normalized_gradient, -1, keepdims=True))) / norms
    raw_low = raw_grad.astype(jnp.bfloat16)
    grad_w_out = jnp.dot(pooled_act.T, raw_low, preferred_element_type=jnp.float32)
    pool_grad = jnp.dot(raw_low, student_w_out.T, preferred_element_type=jnp.float32)
    scale_blocks = (pool_grad / counts).reshape(N_DP, DOC_DEV, FF_S)

    def backward_block(total, triple):
        block, mask, scale = triple
        tokens = layer_norm(block, student_ln_gain).reshape(DOC_DEV * SEQ, D_S)
        pre_act = jnp.dot(tokens, student_w_in, preferred_element_type=jnp.float32)
        slope = gelu_slope(pre_act).reshape(DOC_DEV, SEQ, FF_S)
        act_grad = (slope * mask[:, :, None] * scale[:, None, :]).astype(jnp.bfloat16).reshape(DOC_DEV * SEQ, FF_S)
        return (total + jnp.dot(tokens.T, act_grad, preferred_element_type=jnp.float32), None)
    grad_w_in, unused = lax.scan(backward_block, jnp.zeros((D_S, FF_S), jnp.float32), (state_blocks, mask_blocks, scale_blocks))
    return (loss, grad_w_in, grad_w_out, teacher_states)
```

```python
import jax
import jax.numpy as jnp
from jax import lax
from jax.sharding import PartitionSpec as P

student_softness = 0.05
teacher_softness = 0.02


def layer_norm(states, gain):
    values = states.astype(jnp.float32)
    center = values - jnp.mean(values, -1, keepdims=True)
    spread = jnp.mean(center * center, -1, keepdims=True)
    return (center * lax.rsqrt(spread + 1e-05) * gain).astype(jnp.bfloat16)


def gelu_exact(value):
    return 0.5 * value * (1.0 + jax.scipy.special.erf(value * 0.7071067811865476))


def gelu_slope(value):
    return (
        0.5 * (1.0 + jax.scipy.special.erf(value * 0.7071067811865476))
        + value * jnp.exp(-0.5 * value * value) * 0.3989422804014327
    )


def contrast(student_logits, teacher_logits, row_ids, col_ids):
    keep = row_ids[:, None] != col_ids[None, :]
    partner = (row_ids + 1 - 2 * (row_ids % 2))[:, None] == col_ids[None, :]
    s_exp = jnp.where(keep, jnp.exp(student_logits), 0.0)
    t_exp = jnp.where(keep, jnp.exp(teacher_logits), 0.0)
    s_total = jnp.sum(s_exp, -1, keepdims=True)
    t_total = jnp.sum(t_exp, -1, keepdims=True)
    s_prob = s_exp / s_total
    t_prob = t_exp / t_total
    s_log = student_logits - jnp.log(s_total)
    t_log = teacher_logits - jnp.log(t_total)
    terms = jnp.where(partner, -s_log, 0.0) + jnp.where(keep, t_prob * (t_log - s_log), 0.0)
    gradient_list = 2.0 * s_prob - partner.astype(jnp.float32) - t_prob
    return (gradient_list, jnp.sum(terms))


def exchange(blocks, axis):
    return lax.all_to_all(blocks, axis, 0, 0, tiled=True)


def gather(value, axis):
    count = lax.axis_size(axis)
    return exchange(jnp.broadcast_to(value[None], (count,) + value.shape), axis)


def on_device(
    student_states,
    lengths,
    student_ln_gain,
    student_w_in,
    student_w_out,
    teacher_rows,
    teacher_mlp_gain,
    teacher_gate_up,
    teacher_down,
    teacher_final_gain,
):
    f32, bf16 = jnp.float32, jnp.bfloat16
    dp_count = lax.axis_size("dp")
    section_count = lax.axis_size("section")
    dp_index = lax.axis_index("dp")
    section_index = lax.axis_index("section")
    local_docs = teacher_rows.shape[0]
    total_docs = local_docs * dp_count
    highest = lax.Precision.HIGHEST
    col_width = teacher_gate_up.shape[1]
    hidden_width = teacher_gate_up.shape[2]

    rows_f = teacher_rows.astype(f32)
    inverse = lax.rsqrt(jnp.mean(rows_f * rows_f, -1, keepdims=True) + 1e-06)
    normed = (rows_f * inverse * teacher_mlp_gain).astype(bf16)
    both_rows = jnp.stack([normed, teacher_rows]).reshape(2, local_docs, dp_count, col_width)
    columns = exchange(both_rows.transpose(2, 0, 1, 3), "dp")
    normed_columns = columns[:, 0].reshape(total_docs, col_width)
    row_columns = columns[:, 1].reshape(total_docs, col_width).astype(f32)
    gate_part = jnp.dot(normed_columns, teacher_gate_up[0], preferred_element_type=f32)
    upper_part = jnp.dot(normed_columns, teacher_gate_up[1], preferred_element_type=f32)
    parts = jnp.concatenate([gate_part.astype(bf16), upper_part.astype(bf16)], axis=1)
    parts = exchange(parts.reshape(dp_count, local_docs, 2 * hidden_width), "dp")
    both = jnp.sum(parts.astype(f32), 0)
    hidden = (jax.nn.silu(both[:, :hidden_width]) * both[:, hidden_width:]).astype(bf16)
    every_hidden = gather(hidden, "dp").reshape(total_docs, hidden_width)
    partial_out = jnp.dot(every_hidden, teacher_down, preferred_element_type=f32)
    mlp_part = jnp.sum(gather(partial_out.astype(bf16), "section").astype(f32), 0)
    states_block = row_columns + mlp_part
    final_gain = lax.dynamic_slice_in_dim(teacher_final_gain, dp_index * col_width, col_width, 0)
    scaled = states_block * final_gain
    gram_part = lax.dot_general(
        scaled, scaled, (((1,), (1,)), ((), ())), precision=highest, preferred_element_type=f32
    )
    gram = jnp.sum(gather(gram_part, "dp"), 0)
    squares = jnp.diagonal(gram)
    teacher_norms = jnp.sqrt(squares + 1e-06)
    teacher_logits = gram / (teacher_norms[:, None] * teacher_norms[None, :]) / teacher_softness
    by_block = exchange(states_block.reshape(dp_count, local_docs, col_width), "dp")
    per_section = dp_count // section_count
    own_blocks = lax.dynamic_slice_in_dim(by_block, section_index * per_section, per_section, 0)
    teacher_states = own_blocks.transpose(1, 0, 2).reshape(local_docs, per_section * col_width)

    seq_len = student_states.shape[1]
    width = student_states.shape[2]
    tokens = layer_norm(student_states, student_ln_gain).reshape(local_docs * seq_len, width)
    pre_act = jnp.dot(tokens, student_w_in, preferred_element_type=f32)
    act = gelu_exact(pre_act).astype(bf16).reshape(local_docs, seq_len, -1)
    positions = jnp.arange(seq_len, dtype=jnp.int32)
    mask_f = (positions[None, :] < lengths[:, None]).astype(f32)
    mask_low = mask_f.astype(bf16)
    counts = lengths.astype(f32)[:, None]
    pooled_act = (
        jnp.einsum("bs,bsf->bf", mask_low, act, preferred_element_type=f32) / counts
    ).astype(bf16)
    pooled_x = (
        jnp.einsum("bs,bse->be", mask_low, student_states, preferred_element_type=f32) / counts
    )
    partial_emb = jnp.dot(pooled_act, student_w_out, preferred_element_type=f32)
    student_raw = pooled_x + jnp.sum(gather(partial_emb, "section"), 0)
    all_raw = gather(student_raw, "dp").reshape(total_docs, width)
    norms = jnp.sqrt(jnp.sum(all_raw * all_raw, -1, keepdims=True) + 1e-06)
    unit = all_raw / norms
    student_logits = (
        lax.dot_general(
            unit, unit, (((1,), (1,)), ((), ())), precision=highest, preferred_element_type=f32
        )
        / student_softness
    )
    ids = jnp.arange(total_docs, dtype=jnp.int32)
    gradient_list, loss = contrast(student_logits, teacher_logits, ids, ids)
    unit_grad = (
        jnp.dot(gradient_list + gradient_list.T, unit, precision=highest) / student_softness
    )
    raw_grad = (unit_grad - unit * jnp.sum(unit * unit_grad, -1, keepdims=True)) / norms
    every_low = raw_grad.astype(bf16)
    raw_low = lax.dynamic_slice_in_dim(every_low, dp_index * local_docs, local_docs, 0)

    pooled_columns = exchange(
        pooled_act.reshape(local_docs, dp_count, -1).transpose(1, 0, 2), "dp"
    ).reshape(total_docs, -1)
    grad_w_out = lax.dot_general(
        pooled_columns, every_low, (((0,), (0,)), ((), ())), preferred_element_type=f32
    )

    pool_grad = lax.dot_general(
        raw_low, student_w_out, (((1,), (1,)), ((), ())), preferred_element_type=f32
    )
    scale = pool_grad / counts
    slope = gelu_slope(pre_act).reshape(local_docs, seq_len, -1)
    act_grad = (
        (slope * mask_f[:, :, None] * scale[:, None, :])
        .astype(bf16)
        .reshape(local_docs * seq_len, -1)
    )
    grad_part = lax.dot_general(
        tokens, act_grad, (((0,), (0,)), ((), ())), preferred_element_type=f32
    )
    grad_part = grad_part.astype(bf16).reshape(dp_count, width // dp_count, -1)
    grad_w_in = jnp.sum(exchange(grad_part, "dp").astype(f32), 0)
    return (loss, grad_w_in, grad_w_out, teacher_states)


def solution(mesh):
    placed = (
        P("dp", None, None),
        P("dp"),
        P(),
        P(None, "section"),
        P("section", None),
        P("dp", None),
        P(),
        P(None, "dp", "section"),
        P("section", "dp"),
        P(),
    )
    return jax.shard_map(
        on_device,
        mesh=mesh,
        in_specs=placed,
        out_specs=(P(), P("dp", "section"), P(("section", "dp"), None), P("dp", "section")),
        check_vma=False,
    )
```

```python
import functools

import jax
import jax.numpy as jnp
from jax import lax
from jax.experimental import pallas as pl
from jax.experimental.pallas import tpu as pltpu
from jax.sharding import PartitionSpec as P


student_softness = 0.05
teacher_softness = 0.02
f32 = jnp.float32
bf16 = jnp.bfloat16
highest = lax.Precision.HIGHEST


def exchange(blocks, axis):
    return lax.all_to_all(blocks, axis, 0, 0, tiled=True)


def swap(value, axis, bit):
    members = lax.axis_size(axis)
    return lax.ppermute(value, axis, [(i, i ^ (1 << bit)) for i in range(members)])


def student_doc(rows, length, states, gain, w_in, grad, pool_act, pool_x):
    low = states[0, :rows, :]
    values = low.astype(f32)
    center = values - jnp.mean(values, -1, keepdims=True)
    spread = jnp.mean(center * center, -1, keepdims=True)
    real = lax.broadcasted_iota(jnp.int32, (rows, 1), 0) < length
    inverse = jnp.where(real, lax.rsqrt(spread + 1e-05), 0.0)
    tokens = (center * inverse * gain[...]).astype(bf16)
    real = lax.broadcasted_iota(jnp.int32, (8, rows), 1) < length
    sums = jnp.dot(real.astype(bf16), low, preferred_element_type=f32)
    count = length.astype(f32)
    pool_x[0] = sums[:1] / count
    pre_act = jnp.dot(tokens, w_in[...], preferred_element_type=f32)
    half_erf = 0.5 * (1.0 + lax.erf(pre_act * 0.7071067811865476))
    act = (pre_act * half_erf).astype(bf16)
    bell = jnp.exp(-0.5 * pre_act * pre_act)
    slope = (half_erf + pre_act * bell * 0.3989422804014327).astype(bf16)
    sums = jnp.dot(jnp.ones((8, rows), bf16), act, preferred_element_type=f32)
    pool_act[0] = sums[:1] / count
    product = lax.dot_general(
        tokens, slope, (((0,), (0,)), ((), ())), preferred_element_type=f32
    )
    grad[0] = product.astype(bf16)


def student_kernel(first_doc, lens, states, gain, w_in, after, grad, pool_act, pool_x):
    length = lens[first_doc + pl.program_id(0)]
    seq_len = states.shape[1]
    refs = (states, gain, w_in, grad, pool_act, pool_x)
    few = seq_len // 2 if seq_len % 256 == 0 else seq_len

    @pl.when(length <= few)
    def _():
        student_doc(few, length, *refs)

    @pl.when(length > few)
    def _():
        student_doc(seq_len, length, *refs)


def student_part(lengths, states, gain, w_in, after, first_doc, docs):
    seq_len, width = states.shape[1:]
    hidden = w_in.shape[1]
    return pl.pallas_call(
        functools.partial(student_kernel, first_doc),
        grid_spec=pltpu.PrefetchScalarGridSpec(
            num_scalar_prefetch=1,
            grid=(docs,),
            in_specs=[
                pl.BlockSpec((1, seq_len, width), lambda i, n: (first_doc + i, 0, 0)),
                pl.BlockSpec((1, width), lambda i, n: (0, 0)),
                pl.BlockSpec((width, hidden), lambda i, n: (0, 0)),
                pl.BlockSpec(memory_space=pl.ANY),
            ],
            out_specs=[
                pl.BlockSpec((1, width, hidden), lambda i, n: (i, 0, 0)),
                pl.BlockSpec((1, 1, hidden), lambda i, n: (i, 0, 0)),
                pl.BlockSpec((1, 1, width), lambda i, n: (i, 0, 0)),
            ],
        ),
        out_shape=[
            jax.ShapeDtypeStruct((docs, width, hidden), bf16),
            jax.ShapeDtypeStruct((docs, 1, hidden), f32),
            jax.ShapeDtypeStruct((docs, 1, width), f32),
        ],
        compiler_params=pltpu.CompilerParams(
            dimension_semantics=("arbitrary",), vmem_limit_bytes=60 << 20
        ),
        cost_estimate=pl.CostEstimate(
            flops=3 * docs * seq_len * width * hidden,
            bytes_accessed=docs * width * (seq_len + hidden) * 2,
            transcendentals=docs * seq_len * hidden,
        ),
        name="student",
    )(lengths, states, gain.reshape(1, width), w_in, after)


def gate_up_kernel(block, place, columns, gain, weights, parts, held, arrived):
    hidden = weights.shape[2]
    copies = []
    for i in range(hidden // block):
        here = pl.ds(i * block, block)
        copies.append(
            pltpu.make_async_copy(weights.at[:, :, here], held.at[:, :, here], arrived.at[i])
        )
        copies[-1].start()
    depth = columns.shape[1]
    factors = gain[:, pl.ds(pl.multiple_of(place[0] * depth, depth), depth)]
    scaled = (columns[...].astype(f32) * factors).astype(bf16)
    for i, copy in enumerate(copies):
        copy.wait()
        for side in range(2):
            part = jnp.dot(
                scaled, held[side, :, i * block : (i + 1) * block], preferred_element_type=f32
            )
            first = (2 * i + side) * block
            parts[:, first : first + block] = part.astype(bf16)


def gate_up(place, columns, gain, weights, block):
    hidden = weights.shape[2]
    vmem = pl.BlockSpec(memory_space=pltpu.VMEM)
    return pl.pallas_call(
        functools.partial(gate_up_kernel, block),
        in_specs=[
            pl.BlockSpec(memory_space=pltpu.SMEM),
            vmem,
            vmem,
            pl.BlockSpec(memory_space=pltpu.HBM),
        ],
        out_specs=vmem,
        out_shape=jax.ShapeDtypeStruct((columns.shape[0], 2 * hidden), bf16),
        scratch_shapes=[
            pltpu.VMEM(weights.shape, bf16),
            pltpu.SemaphoreType.DMA((hidden // block,)),
        ],
        compiler_params=pltpu.CompilerParams(vmem_limit_bytes=24 << 20),
        name="gate_up",
    )(place, columns, gain.reshape(1, -1), weights)


def hidden_kernel(block, parts, rows, hidden):
    row = rows[...].astype(f32)
    inverse = lax.rsqrt(jnp.mean(row * row, -1, keepdims=True) + 1e-06)
    for first in range(0, hidden.shape[2], block):
        both = jnp.sum(parts[:, :, 2 * first : 2 * (first + block)].astype(f32), 0) * inverse
        gate, upper = both[:, :block], both[:, block:]
        value = (gate / (1.0 + jnp.exp(-gate)) * upper).astype(bf16)
        for copy in range(hidden.shape[0]):
            hidden[copy, :, first : first + block] = value


def hidden_units(parts, rows, block):
    members, docs, both = parts.shape
    return pl.pallas_call(
        functools.partial(hidden_kernel, block),
        out_shape=jax.ShapeDtypeStruct((members, docs, both // 2), bf16),
        compiler_params=pltpu.CompilerParams(vmem_limit_bytes=12 << 20),
        name="hidden",
    )(parts, rows)


def down_kernel(block, hidden, weights, out, held, arrived):
    copies = []
    for i in range(weights.shape[0] // block):
        here = pl.ds(i * block, block)
        copies.append(pltpu.make_async_copy(weights.at[here], held.at[here], arrived.at[i]))
        copies[-1].start()
    total = None
    for i, copy in enumerate(copies):
        copy.wait()
        here = slice(i * block, (i + 1) * block)
        part = jnp.dot(hidden[:, here], held[here, :], preferred_element_type=f32)
        total = part if total is None else total + part
    out[...] = total


def down(hidden, weights, block):
    vmem = pl.BlockSpec(memory_space=pltpu.VMEM)
    return pl.pallas_call(
        functools.partial(down_kernel, block),
        in_specs=[vmem, pl.BlockSpec(memory_space=pltpu.HBM)],
        out_specs=vmem,
        out_shape=jax.ShapeDtypeStruct((hidden.shape[0], weights.shape[1]), f32),
        scratch_shapes=[
            pltpu.VMEM(weights.shape, bf16),
            pltpu.SemaphoreType.DMA((weights.shape[0] // block,)),
        ],
        compiler_params=pltpu.CompilerParams(vmem_limit_bytes=20 << 20),
        name="down",
    )(hidden, weights)


def states_kernel(place, kept, arrived, columns, gain, states, gram):
    value = columns[...].astype(f32) + (kept[...].astype(f32) + arrived[...].astype(f32))
    states[...] = value
    width = value.shape[1]
    scaled = value * gain[:, pl.ds(pl.multiple_of(place[0] * width, width), width)]
    product = lax.dot_general(
        scaled, scaled, (((1,), (1,)), ((), ())), precision=highest, preferred_element_type=f32
    )
    rows = gram.shape[0]
    packed = [product[i : i + rows] for i in range(0, product.shape[0], rows)]
    gram[...] = packed[0] if len(packed) == 1 else jnp.concatenate(packed, axis=1)


def packed_rows(docs):
    return docs * docs // 128 if docs < 128 and 128 % docs == 0 else docs


def teacher_block(place, kept, arrived, columns, gain):
    docs, width = columns.shape
    rows = packed_rows(docs)
    vmem = pl.BlockSpec(memory_space=pltpu.VMEM)
    return pl.pallas_call(
        states_kernel,
        in_specs=[pl.BlockSpec(memory_space=pltpu.SMEM)] + [vmem] * 4,
        out_specs=[vmem] * 2,
        out_shape=[
            jax.ShapeDtypeStruct((docs, width), f32),
            jax.ShapeDtypeStruct((rows, docs * docs // rows), f32),
        ],
        compiler_params=pltpu.CompilerParams(vmem_limit_bytes=8 << 20),
        name="teacher_block",
    )(place, kept, arrived, columns, gain.reshape(1, -1))


def embed_kernel(order, place, blocks, unit, norms, logits, raw):
    docs = blocks.shape[1]
    for i in range(blocks.shape[0]):
        member = place[0] ^ sum(((i >> k) & 1) << bit for k, bit in enumerate(order))
        raw[pl.ds(pl.multiple_of(member * docs, docs), docs), :] = blocks[i]
    value = raw[...]
    size = jnp.sqrt(jnp.sum(value * value, -1, keepdims=True) + 1e-06)
    units = value / size
    norms[...] = size
    unit[...] = units
    logits[...] = (
        lax.dot_general(
            units, units, (((1,), (1,)), ((), ())), precision=highest, preferred_element_type=f32
        )
        / student_softness
    )


def embed(place, blocks, order):
    members, each, width = blocks.shape
    docs = members * each
    vmem = pl.BlockSpec(memory_space=pltpu.VMEM)
    return pl.pallas_call(
        functools.partial(embed_kernel, order),
        in_specs=[pl.BlockSpec(memory_space=pltpu.SMEM), vmem],
        out_specs=[vmem] * 3,
        out_shape=[
            jax.ShapeDtypeStruct((docs, width), f32),
            jax.ShapeDtypeStruct((docs, 1), f32),
            jax.ShapeDtypeStruct((docs, docs), f32),
        ],
        scratch_shapes=[pltpu.VMEM((docs, width), f32)],
        compiler_params=pltpu.CompilerParams(vmem_limit_bytes=8 << 20),
        name="embed",
    )(place, blocks)


def contrast_kernel(place, lens, gram_sum, logits, unit, norms, w_out, *refs):
    loss, low, scale, raw = refs[-4:]
    gram = gram_sum[...]
    docs = logits.shape[0]
    if gram.shape[1] != docs:
        gram = jnp.concatenate(
            [gram[:, i : i + docs] for i in range(0, gram.shape[1], docs)], axis=0
        )
    row = lax.broadcasted_iota(jnp.int32, (docs, docs), 0)
    col = lax.broadcasted_iota(jnp.int32, (docs, docs), 1)
    keep = row != col
    partner = (row + 1 - 2 * (row % 2)) == col
    own = jnp.where(keep, 0.0, gram)
    sizes_down = jnp.sqrt(jnp.sum(own, 1, keepdims=True) + 1e-06)
    sizes_along = jnp.sqrt(jnp.sum(own, 0, keepdims=True) + 1e-06)
    t_logits = gram / (sizes_down * sizes_along) / teacher_softness
    s_logits = logits[...]
    t_exp = jnp.where(keep, jnp.exp(t_logits), 0.0)
    s_exp = jnp.where(keep, jnp.exp(s_logits), 0.0)
    t_down = jnp.sum(t_exp, 1, keepdims=True)
    s_down = jnp.sum(s_exp, 1, keepdims=True)
    t_along = jnp.sum(t_exp, 0, keepdims=True)
    s_along = jnp.sum(s_exp, 0, keepdims=True)
    s_log = s_logits - jnp.log(s_down)
    t_log = t_logits - jnp.log(t_down)
    terms = jnp.where(partner, -s_log, 0.0)
    terms = terms + jnp.where(keep, t_exp / t_down * (t_log - s_log), 0.0)
    loss[...] = jnp.sum(jnp.sum(terms, 1, keepdims=True), 0, keepdims=True)
    both = 2.0 * (s_exp / s_down + s_exp / s_along) - (t_exp / t_down + t_exp / t_along)
    both = both - jnp.where(partner, 2.0, 0.0)
    units = unit[...]
    unit_grad = (
        jnp.dot(both, units, precision=highest, preferred_element_type=f32) / student_softness
    )
    along = jnp.sum(units * unit_grad, -1, keepdims=True)
    raw_low = ((unit_grad - units * along) / norms[...]).astype(bf16)
    low[...] = raw_low
    raw[...] = raw_low.astype(f32)
    mine = raw[pl.ds(pl.multiple_of(place[0] * scale.shape[0], scale.shape[0]), scale.shape[0]), :]
    pool_grad = lax.dot_general(
        mine.astype(bf16), w_out[...], (((1,), (1,)), ((), ())), preferred_element_type=f32
    )
    for doc in range(scale.shape[0]):
        scale[doc : doc + 1, :] = pool_grad[doc : doc + 1, :] / lens[doc].astype(f32)


def contrast(place, lengths, gram_sum, logits, unit, norms, w_out, *after):
    total_docs, width = unit.shape
    local_docs, hidden = lengths.shape[0], w_out.shape[0]
    vmem, smem = pl.BlockSpec(memory_space=pltpu.VMEM), pl.BlockSpec(memory_space=pltpu.SMEM)
    return pl.pallas_call(
        contrast_kernel,
        in_specs=[smem] * 2 + [vmem] * 5 + [pl.BlockSpec(memory_space=pl.ANY)] * len(after),
        out_specs=[vmem] * 3,
        out_shape=[
            jax.ShapeDtypeStruct((1, 1), f32),
            jax.ShapeDtypeStruct((total_docs, width), bf16),
            jax.ShapeDtypeStruct((local_docs, hidden), f32),
        ],
        scratch_shapes=[pltpu.VMEM((total_docs, width), f32)],
        compiler_params=pltpu.CompilerParams(vmem_limit_bytes=20 << 20),
        name="contrast",
    )(place, lengths, gram_sum, logits, unit, norms, w_out, *after)


def relative(order, bits, step):
    return sum(((step >> (bits - 1 - k)) & 1) << bit for k, bit in enumerate(order))


def weigh_kernel(orders, bits, first, parts, place, scale, *refs):
    grads, outs = refs[:parts], refs[-2:]
    half, rows, group = scale.shape[1] // 2, outs[0].shape[1], 16
    for side in range(2):
        here = pl.ds(side * half, half)
        factors = scale[:, side * half : (side + 1) * half]
        member = place[0] ^ relative(orders[side], bits, first + pl.program_id(0))
        start = pl.multiple_of(member * rows, rows)

        def step(i, carry, side=side, here=here, factors=factors, start=start):
            near = pl.multiple_of(i * group, group)
            total, doc = None, 0
            for grad in grads:
                for j in range(grad.shape[0]):
                    value = grad[j, pl.ds(start + near, group), here].astype(f32)
                    term = value * factors[doc : doc + 1]
                    total = term if total is None else total + term
                    doc += 1
            outs[side][0, pl.ds(near, group), :] = total.astype(bf16)
            return carry

        lax.fori_loop(0, rows // group, step, 0)


def weigh(place, scale, grads, orders, members, first, after=()):
    width, hidden = grads[0].shape[1:]
    bits = members.bit_length() - 1
    rows, half = width // members, hidden // 2
    vmem = pl.BlockSpec(memory_space=pltpu.VMEM)
    return pl.pallas_call(
        functools.partial(weigh_kernel, orders, bits, first, len(grads)),
        grid_spec=pltpu.PrefetchScalarGridSpec(
            num_scalar_prefetch=1,
            grid=(members // 2,),
            in_specs=[pl.BlockSpec(scale.shape, lambda i, p: (0, 0))]
            + [vmem] * len(grads)
            + [pl.BlockSpec(memory_space=pl.ANY)] * len(after),
            out_specs=[pl.BlockSpec((1, rows, half), lambda i, p: (i, 0, 0))] * 2,
        ),
        out_shape=[jax.ShapeDtypeStruct((members // 2, rows, half), bf16)] * 2,
        compiler_params=pltpu.CompilerParams(
            dimension_semantics=("arbitrary",), vmem_limit_bytes=24 << 20
        ),
        name="weigh",
    )(place, scale, *grads, *after)


def halving(sent, kept, order, axis):
    for bit in order:
        arrived = swap(sent, axis, bit)
        rest = kept.shape[0] // 2
        if rest:
            sent = (kept[rest:].astype(f32) + arrived[rest:].astype(f32)).astype(bf16)
            kept = (kept[:rest].astype(f32) + arrived[:rest].astype(f32)).astype(bf16)
    return kept[0].astype(f32) + arrived[0].astype(f32)


def on_device(
    student_states,
    lengths,
    student_ln_gain,
    student_w_in,
    student_w_out,
    teacher_rows,
    teacher_mlp_gain,
    teacher_gate_up,
    teacher_down,
    teacher_final_gain,
):
    dp_count = lax.axis_size("dp")
    section_count = lax.axis_size("section")
    dp_index = lax.axis_index("dp")
    section_index = lax.axis_index("section")
    local_docs = teacher_rows.shape[0]
    total_docs = local_docs * dp_count
    col_width = teacher_gate_up.shape[1]
    hidden_width = teacher_gate_up.shape[2]
    place = dp_index.astype(jnp.int32).reshape(1)
    block = hidden_width // 6 if hidden_width % 768 == 0 else hidden_width
    student = functools.partial(
        student_part, lengths, student_states, student_ln_gain, student_w_in
    )
    cuts = (0, local_docs // 4, local_docs - local_docs // 8, local_docs)

    blocks = teacher_rows.reshape(local_docs, dp_count, col_width).transpose(1, 0, 2)
    columns = exchange(blocks, "dp").reshape(total_docs, col_width)
    first = student(teacher_rows, cuts[0], cuts[1] - cuts[0])
    parts = gate_up(place, columns, teacher_mlp_gain, teacher_gate_up, block)
    parts = parts.reshape(dp_count, local_docs, 2 * hidden_width)
    second = student(parts, cuts[1], cuts[2] - cuts[1])
    parts = exchange(parts, "dp")
    hidden = hidden_units(parts, teacher_rows, block)
    third = student(hidden, cuts[2], cuts[3] - cuts[2])
    every_hidden = exchange(hidden, "dp").reshape(total_docs, hidden_width)
    out = down(every_hidden, teacher_down, block)
    for bit in range(section_count.bit_length() - 1):
        kept = out if bit == 0 else out.astype(bf16)
        arrived = swap(kept, "section", bit)
        out = kept.astype(f32) + arrived.astype(f32)
    states_block, gram_sum = teacher_block(place, kept, arrived, columns, teacher_final_gain)
    bits = dp_count.bit_length() - 1
    for bit in range(bits):
        gram_sum = gram_sum + swap(gram_sum, "dp", bit)

    grads, acts, states = zip(first, second, third)
    pooled_act = jnp.concatenate(acts)[:, 0].astype(bf16)
    pooled_x = jnp.concatenate(states)[:, 0]
    emb_sum = jnp.dot(pooled_act, student_w_out, preferred_element_type=f32)
    for bit in range(section_count.bit_length() - 1):
        emb_sum = emb_sum + swap(emb_sum, "section", bit)
    far_first = tuple(reversed(range(bits)))
    every_raw = (pooled_x + emb_sum)[None]
    for bit in far_first:
        every_raw = jnp.concatenate([every_raw, swap(every_raw, "dp", bit)])
    unit, norms, student_logits = embed(place, every_raw, far_first)
    loss, every_low, scale = contrast(
        place, lengths, gram_sum, student_logits, unit, norms, student_w_out
    )

    orders = (tuple(range(bits)), (1, 0) + tuple(range(2, bits)))
    sent = weigh(place, scale, grads, orders, dp_count, dp_count // 2)
    kept = weigh(place, scale, grads, orders, dp_count, 0, sent)
    sides = []
    for side in range(2):
        sides.append(halving(sent[side], kept[side], orders[side], "dp"))
    grad_w_in = jnp.concatenate(sides, axis=1)
    pooled = pooled_act.reshape(local_docs, dp_count, -1).transpose(1, 0, 2).astype(f32)
    states_block = states_block.reshape(dp_count, local_docs, col_width)
    last = exchange(jnp.concatenate([states_block, pooled], axis=2), "dp")
    per_section = dp_count // section_count
    own_blocks = lax.dynamic_slice_in_dim(last, section_index * per_section, per_section, 0)
    own_blocks = own_blocks[:, :, :col_width].transpose(1, 0, 2)
    teacher_states = own_blocks.reshape(local_docs, per_section * col_width)
    pooled_columns = last[:, :, col_width:].reshape(total_docs, -1).astype(bf16)
    grad_w_out = lax.dot_general(
        pooled_columns, every_low, (((0,), (0,)), ((), ())), preferred_element_type=f32
    )
    return (loss[0, 0], grad_w_in, grad_w_out, teacher_states)


def solution(mesh):
    placed = (
        P("dp", None, None),
        P("dp"),
        P(),
        P(None, "section"),
        P("section", None),
        P("dp", None),
        P(),
        P(None, "dp", "section"),
        P("section", "dp"),
        P(),
    )

    return jax.shard_map(
        on_device,
        mesh=mesh,
        in_specs=placed,
        out_specs=(P(), P("dp", "section"), P(("section", "dp"), None), P("dp", "section")),
        check_vma=False,
    )
```

```python
import functools

import jax
import jax.numpy as jnp
from jax import lax
from jax.experimental import pallas as pl
from jax.experimental.pallas import tpu as pltpu
from jax.sharding import PartitionSpec as P


student_softness = 0.05
teacher_softness = 0.02
f32 = jnp.float32
bf16 = jnp.bfloat16
highest = lax.Precision.HIGHEST


def exchange(blocks, axis):
    return lax.all_to_all(blocks, axis, 0, 0, tiled=True)


def swap(value, axis, bit):
    members = lax.axis_size(axis)
    return lax.ppermute(value, axis, [(i, i ^ (1 << bit)) for i in range(members)])


def student_doc(rows, length, states, gain, w_in, grad, pool_act, pool_x):
    low = states[0, :rows, :]
    values = low.astype(f32)
    center = values - jnp.mean(values, -1, keepdims=True)
    spread = jnp.mean(center * center, -1, keepdims=True)
    real = lax.broadcasted_iota(jnp.int32, (rows, 1), 0) < length
    inverse = jnp.where(real, lax.rsqrt(spread + 1e-05), 0.0)
    tokens = (center * inverse * gain[...]).astype(bf16)
    real = lax.broadcasted_iota(jnp.int32, (8, rows), 1) < length
    sums = jnp.dot(real.astype(bf16), low, preferred_element_type=f32)
    count = length.astype(f32)
    pool_x[0] = sums[:1] / count
    pre_act = jnp.dot(tokens, w_in[...], preferred_element_type=f32)
    half_erf = 0.5 * (1.0 + lax.erf(pre_act * 0.7071067811865476))
    act = (pre_act * half_erf).astype(bf16)
    bell = jnp.exp(-0.5 * pre_act * pre_act)
    slope = (half_erf + pre_act * bell * 0.3989422804014327).astype(bf16)
    pool_act[0] = jnp.sum(act.astype(f32), 0, keepdims=True) / count
    product = lax.dot_general(
        tokens, slope, (((0,), (0,)), ((), ())), preferred_element_type=f32
    )
    half = grad.shape[3]
    for side in range(grad.shape[1]):
        grad[0, side] = product[:, side * half : (side + 1) * half].astype(bf16)


def student_kernel(first_doc, lens, states, gain, w_in, after, grad, pool_act, pool_x):
    length = lens[first_doc + pl.program_id(0)]
    seq_len = states.shape[1]
    refs = (states, gain, w_in, grad, pool_act, pool_x)
    few = seq_len // 2 if seq_len % 256 == 0 else seq_len

    @pl.when(length <= few)
    def _():
        student_doc(few, length, *refs)

    @pl.when(length > few)
    def _():
        student_doc(seq_len, length, *refs)


def student_part(lengths, states, gain, w_in, after, first_doc, docs):
    seq_len, width = states.shape[1:]
    hidden = w_in.shape[1]
    return pl.pallas_call(
        functools.partial(student_kernel, first_doc),
        grid_spec=pltpu.PrefetchScalarGridSpec(
            num_scalar_prefetch=1,
            grid=(docs,),
            in_specs=[
                pl.BlockSpec((1, seq_len, width), lambda i, n: (first_doc + i, 0, 0)),
                pl.BlockSpec((1, width), lambda i, n: (0, 0)),
                pl.BlockSpec((width, hidden), lambda i, n: (0, 0)),
                pl.BlockSpec(memory_space=pl.ANY),
            ],
            out_specs=[
                pl.BlockSpec((1, 2, width, hidden // 2), lambda i, n: (i, 0, 0, 0)),
                pl.BlockSpec((1, 1, hidden), lambda i, n: (i, 0, 0)),
                pl.BlockSpec((1, 1, width), lambda i, n: (i, 0, 0)),
            ],
        ),
        out_shape=[
            jax.ShapeDtypeStruct((docs, 2, width, hidden // 2), bf16),
            jax.ShapeDtypeStruct((docs, 1, hidden), f32),
            jax.ShapeDtypeStruct((docs, 1, width), f32),
        ],
        compiler_params=pltpu.CompilerParams(
            dimension_semantics=("arbitrary",), vmem_limit_bytes=59 << 20
        ),
        cost_estimate=pl.CostEstimate(
            flops=3 * docs * seq_len * width * hidden,
            bytes_accessed=docs * width * (seq_len + hidden) * 2,
            transcendentals=docs * seq_len * hidden,
        ),
        name="student",
    )(lengths, states, gain.reshape(1, width), w_in, after)


def gate_up_kernel(block, place, columns, gain, weights, parts, held, arrived):
    hidden = weights.shape[2]
    copies = []
    for i in range(hidden // block):
        here = pl.ds(i * block, block)
        copies.append(
            pltpu.make_async_copy(weights.at[:, :, here], held.at[:, :, here], arrived.at[i])
        )
        copies[-1].start()
    depth = columns.shape[1]
    factors = gain[:, pl.ds(pl.multiple_of(place[0] * depth, depth), depth)]
    scaled = (columns[...].astype(f32) * factors).astype(bf16)
    for i, copy in enumerate(copies):
        copy.wait()
        for side in range(2):
            part = jnp.dot(
                scaled, held[side, :, i * block : (i + 1) * block], preferred_element_type=f32
            )
            first = (2 * i + side) * block
            parts[:, first : first + block] = part.astype(bf16)


def gate_up(place, columns, gain, weights, block):
    hidden = weights.shape[2]
    vmem = pl.BlockSpec(memory_space=pltpu.VMEM)
    return pl.pallas_call(
        functools.partial(gate_up_kernel, block),
        in_specs=[
            pl.BlockSpec(memory_space=pltpu.SMEM),
            vmem,
            vmem,
            pl.BlockSpec(memory_space=pltpu.HBM),
        ],
        out_specs=vmem,
        out_shape=jax.ShapeDtypeStruct((columns.shape[0], 2 * hidden), bf16),
        scratch_shapes=[
            pltpu.VMEM(weights.shape, bf16),
            pltpu.SemaphoreType.DMA((hidden // block,)),
        ],
        compiler_params=pltpu.CompilerParams(vmem_limit_bytes=59 << 20),
        name="gate_up",
    )(place, columns, gain.reshape(1, -1), weights)


def hidden_kernel(block, parts, rows, hidden):
    row = rows[...].astype(f32)
    inverse = lax.rsqrt(jnp.mean(row * row, -1, keepdims=True) + 1e-06)
    for first in range(0, hidden.shape[2], block):
        both = jnp.sum(parts[:, :, 2 * first : 2 * (first + block)].astype(f32), 0) * inverse
        gate, upper = both[:, :block], both[:, block:]
        value = (gate / (1.0 + jnp.exp(-gate)) * upper).astype(bf16)
        for copy in range(hidden.shape[0]):
            hidden[copy, :, first : first + block] = value


def hidden_units(parts, rows, block):
    members, docs, both = parts.shape
    return pl.pallas_call(
        functools.partial(hidden_kernel, block),
        out_shape=jax.ShapeDtypeStruct((members, docs, both // 2), bf16),
        compiler_params=pltpu.CompilerParams(vmem_limit_bytes=12 << 20),
        name="hidden",
    )(parts, rows)


def down_kernel(hidden, weights, out):
    out[...] = jnp.dot(hidden[...], weights[...], preferred_element_type=f32)


def down(hidden, weights):
    return pl.pallas_call(
        down_kernel,
        out_shape=jax.ShapeDtypeStruct((hidden.shape[0], weights.shape[1]), f32),
        compiler_params=pltpu.CompilerParams(vmem_limit_bytes=12 << 20),
        name="down",
    )(hidden, weights)


def states_kernel(place, kept, arrived, columns, gain, states, gram):
    value = columns[...].astype(f32) + (kept[...].astype(f32) + arrived[...].astype(f32))
    states[...] = value
    width = value.shape[1]
    scaled = value * gain[:, pl.ds(pl.multiple_of(place[0] * width, width), width)]
    product = lax.dot_general(
        scaled, scaled, (((1,), (1,)), ((), ())), precision=highest, preferred_element_type=f32
    )
    rows = gram.shape[0]
    packed = [product[i : i + rows] for i in range(0, product.shape[0], rows)]
    gram[...] = packed[0] if len(packed) == 1 else jnp.concatenate(packed, axis=1)


def packed_rows(docs):
    return docs * docs // 128 if docs < 128 and 128 % docs == 0 else docs


def teacher_block(place, kept, arrived, columns, gain):
    docs, width = columns.shape
    rows = packed_rows(docs)
    vmem = pl.BlockSpec(memory_space=pltpu.VMEM)
    return pl.pallas_call(
        states_kernel,
        in_specs=[pl.BlockSpec(memory_space=pltpu.SMEM)] + [vmem] * 4,
        out_specs=[vmem] * 2,
        out_shape=[
            jax.ShapeDtypeStruct((docs, width), f32),
            jax.ShapeDtypeStruct((rows, docs * docs // rows), f32),
        ],
        compiler_params=pltpu.CompilerParams(vmem_limit_bytes=8 << 20),
        name="teacher_block",
    )(place, kept, arrived, columns, gain.reshape(1, -1))


def embed_kernel(order, place, blocks, unit, norms, logits, raw):
    docs = blocks.shape[1]
    for i in range(blocks.shape[0]):
        member = place[0] ^ sum(((i >> k) & 1) << bit for k, bit in enumerate(order))
        raw[pl.ds(pl.multiple_of(member * docs, docs), docs), :] = blocks[i]
    value = raw[...]
    size = jnp.sqrt(jnp.sum(value * value, -1, keepdims=True) + 1e-06)
    units = value / size
    norms[...] = size
    unit[...] = units
    logits[...] = (
        lax.dot_general(
            units, units, (((1,), (1,)), ((), ())), precision=highest, preferred_element_type=f32
        )
        / student_softness
    )


def embed(place, blocks, order):
    members, each, width = blocks.shape
    docs = members * each
    vmem = pl.BlockSpec(memory_space=pltpu.VMEM)
    return pl.pallas_call(
        functools.partial(embed_kernel, order),
        in_specs=[pl.BlockSpec(memory_space=pltpu.SMEM), vmem],
        out_specs=[vmem] * 3,
        out_shape=[
            jax.ShapeDtypeStruct((docs, width), f32),
            jax.ShapeDtypeStruct((docs, 1), f32),
            jax.ShapeDtypeStruct((docs, docs), f32),
        ],
        scratch_shapes=[pltpu.VMEM((docs, width), f32)],
        compiler_params=pltpu.CompilerParams(vmem_limit_bytes=8 << 20),
        name="embed",
    )(place, blocks)


def relative(order, step):
    return sum(((step >> (len(order) - 1 - k)) & 1) << bit for k, bit in enumerate(order))


def fetch(plan, place, grads, held, arrived):
    orders, first = plan
    rows = held[0].shape[-2]
    copies = []
    for side, order in enumerate(orders):
        for i in range(held[0].shape[1]):
            member = place[0] ^ relative(order, first + i)
            here = pl.ds(pl.multiple_of(member * rows, rows), rows)
            group = [
                pltpu.make_async_copy(
                    grad.at[:, side, here, :],
                    buffer.at[side, i],
                    arrived.at[part, side, i],
                )
                for part, (grad, buffer) in enumerate(zip(grads, held))
            ]
            for copy in group:
                copy.start()
            copies.append((side, i, group))
    return copies


def weigh_fetched(copies, scale, held, outs):
    half, rows = held[0].shape[-1], held[0].shape[-2]
    lines = 16
    for side, i, group in copies:
        for copy in group:
            copy.wait()
        factors = scale[:, side * half : (side + 1) * half]

        def step(line, carry, side=side, i=i, factors=factors):
            here = pl.ds(pl.multiple_of(line * lines, lines), lines)
            total, doc = None, 0
            for buffer in held:
                for j in range(buffer.shape[2]):
                    term = buffer[side, i, j, here, :].astype(f32) * factors[doc : doc + 1]
                    total = term if total is None else total + term
                    doc += 1
            outs[side][i, here, :] = total.astype(bf16)
            return carry

        lax.fori_loop(0, rows // lines, step, 0)


def block_shapes(grads, members):
    width, half = grads[0].shape[2:]
    rows, count = width // members, members // 2
    buffers = [pltpu.VMEM((2, count, grad.shape[0], rows, half), bf16) for grad in grads]
    arrived = pltpu.SemaphoreType.DMA((len(grads), 2, count))
    return buffers, arrived, [jax.ShapeDtypeStruct((count, rows, half), bf16)] * 2


def contrast_kernel(plan, place, lens, gram_kept, gram_arrived, logits, unit, norms, w_out, *refs):
    parts = (len(refs) - 9) // 2
    grads, refs = refs[:parts], refs[parts:]
    (loss, low, scale), outs, (raw, weights), refs = refs[:3], refs[3:5], refs[5:7], refs[7:]
    held, (weights_here, arrived) = refs[:-2], refs[-2:]
    copy = pltpu.make_async_copy(w_out, weights, weights_here)
    copy.start()
    copies = fetch(plan, place, grads, held, arrived)
    gram = gram_kept[...] + gram_arrived[...]
    docs = logits.shape[0]
    if gram.shape[1] != docs:
        gram = jnp.concatenate(
            [gram[:, i : i + docs] for i in range(0, gram.shape[1], docs)], axis=0
        )
    row = lax.broadcasted_iota(jnp.int32, (docs, docs), 0)
    col = lax.broadcasted_iota(jnp.int32, (docs, docs), 1)
    keep = row != col
    partner = (row + 1 - 2 * (row % 2)) == col
    own = jnp.where(keep, 0.0, gram)
    sizes_down = jnp.sqrt(jnp.sum(own, 1, keepdims=True) + 1e-06)
    sizes_along = jnp.sqrt(jnp.sum(own, 0, keepdims=True) + 1e-06)
    t_logits = gram / (sizes_down * sizes_along) / teacher_softness
    s_logits = logits[...]
    t_exp = jnp.where(keep, jnp.exp(t_logits), 0.0)
    s_exp = jnp.where(keep, jnp.exp(s_logits), 0.0)
    t_down = jnp.sum(t_exp, 1, keepdims=True)
    s_down = jnp.sum(s_exp, 1, keepdims=True)
    t_along = jnp.sum(t_exp, 0, keepdims=True)
    s_along = jnp.sum(s_exp, 0, keepdims=True)
    s_log = s_logits - jnp.log(s_down)
    t_log = t_logits - jnp.log(t_down)
    terms = jnp.where(partner, -s_log, 0.0)
    terms = terms + jnp.where(keep, t_exp / t_down * (t_log - s_log), 0.0)
    loss[...] = jnp.sum(jnp.sum(terms, 1, keepdims=True), 0, keepdims=True)
    both = 2.0 * (s_exp / s_down + s_exp / s_along) - (t_exp / t_down + t_exp / t_along)
    both = both - jnp.where(partner, 2.0, 0.0)
    units = unit[...]
    unit_grad = (
        jnp.dot(both, units, precision=highest, preferred_element_type=f32) / student_softness
    )
    along = jnp.sum(units * unit_grad, -1, keepdims=True)
    raw_low = ((unit_grad - units * along) / norms[...]).astype(bf16)
    low[...] = raw_low
    raw[...] = raw_low.astype(f32)
    mine = raw[pl.ds(pl.multiple_of(place[0] * scale.shape[0], scale.shape[0]), scale.shape[0]), :]
    copy.wait()
    pool_grad = lax.dot_general(
        mine.astype(bf16), weights[...], (((1,), (1,)), ((), ())), preferred_element_type=f32
    )
    for doc in range(scale.shape[0]):
        scale[doc : doc + 1, :] = pool_grad[doc : doc + 1, :] / lens[doc].astype(f32)
    weigh_fetched(copies, scale, held, outs)


def contrast(place, lengths, gram_kept, gram_arrived, logits, unit, norms, w_out, grads, orders, members):
    total_docs, width = unit.shape
    local_docs, hidden = lengths.shape[0], w_out.shape[0]
    buffers, arrived, sums = block_shapes(grads, members)
    vmem, smem = pl.BlockSpec(memory_space=pltpu.VMEM), pl.BlockSpec(memory_space=pltpu.SMEM)
    hbm = pl.BlockSpec(memory_space=pltpu.HBM)
    return pl.pallas_call(
        functools.partial(contrast_kernel, (orders, members // 2)),
        in_specs=[smem] * 2 + [vmem] * 5 + [hbm] * (1 + len(grads)),
        out_specs=[vmem] * 5,
        out_shape=[
            jax.ShapeDtypeStruct((1, 1), f32),
            jax.ShapeDtypeStruct((total_docs, width), bf16),
            jax.ShapeDtypeStruct((local_docs, hidden), f32),
        ]
        + sums,
        scratch_shapes=[pltpu.VMEM((total_docs, width), f32), pltpu.VMEM(w_out.shape, bf16)]
        + buffers
        + [pltpu.SemaphoreType.DMA, arrived],
        compiler_params=pltpu.CompilerParams(vmem_limit_bytes=50 << 20),
        name="contrast",
    )(place, lengths, gram_kept, gram_arrived, logits, unit, norms, w_out, *grads)


def weigh_kernel(plan, parts, place, scale, *refs):
    grads, outs, held, arrived = refs[:parts], refs[-3 - parts : -1 - parts], refs[-1 - parts : -1], refs[-1]
    weigh_fetched(fetch(plan, place, grads, held, arrived), scale, held, outs)


def weigh(place, scale, grads, orders, members, after):
    buffers, arrived, sums = block_shapes(grads, members)
    vmem, smem = pl.BlockSpec(memory_space=pltpu.VMEM), pl.BlockSpec(memory_space=pltpu.SMEM)
    hbm, kept = pl.BlockSpec(memory_space=pltpu.HBM), pl.BlockSpec(memory_space=pl.ANY)
    return pl.pallas_call(
        functools.partial(weigh_kernel, (orders, 0), len(grads)),
        in_specs=[smem, vmem] + [hbm] * len(grads) + [kept] * len(after),
        out_specs=[vmem] * 2,
        out_shape=sums,
        scratch_shapes=buffers + [arrived],
        compiler_params=pltpu.CompilerParams(vmem_limit_bytes=50 << 20),
        name="weigh",
    )(place, scale, *grads, *after)


def halving(sent, kept, order, axis):
    for bit in order:
        arrived = swap(sent, axis, bit)
        rest = kept.shape[0] // 2
        if rest:
            sent = (kept[rest:].astype(f32) + arrived[rest:].astype(f32)).astype(bf16)
            kept = (kept[:rest].astype(f32) + arrived[:rest].astype(f32)).astype(bf16)
    return kept[0].astype(f32) + arrived[0].astype(f32)


def on_device(
    student_states,
    lengths,
    student_ln_gain,
    student_w_in,
    student_w_out,
    teacher_rows,
    teacher_mlp_gain,
    teacher_gate_up,
    teacher_down,
    teacher_final_gain,
):
    dp_count = lax.axis_size("dp")
    section_count = lax.axis_size("section")
    dp_index = lax.axis_index("dp")
    section_index = lax.axis_index("section")
    local_docs = teacher_rows.shape[0]
    total_docs = local_docs * dp_count
    col_width = teacher_gate_up.shape[1]
    hidden_width = teacher_gate_up.shape[2]
    place = dp_index.astype(jnp.int32).reshape(1)
    block = hidden_width // 6 if hidden_width % 768 == 0 else hidden_width
    student = functools.partial(
        student_part, lengths, student_states, student_ln_gain, student_w_in
    )
    early = local_docs // 4

    blocks = teacher_rows.reshape(local_docs, dp_count, col_width).transpose(1, 0, 2)
    columns = exchange(blocks, "dp").reshape(total_docs, col_width)
    first = student(teacher_rows, 0, early)
    parts = gate_up(place, columns, teacher_mlp_gain, teacher_gate_up, block)
    parts = parts.reshape(dp_count, local_docs, 2 * hidden_width)
    second = student(parts, early, local_docs - early)
    parts = exchange(parts, "dp")
    hidden = hidden_units(parts, teacher_rows, block)
    every_hidden = exchange(hidden, "dp").reshape(total_docs, hidden_width)
    out = down(every_hidden, teacher_down)
    for bit in range(section_count.bit_length() - 1):
        kept = out if bit == 0 else out.astype(bf16)
        arrived = swap(kept, "section", bit)
        out = kept.astype(f32) + arrived.astype(f32)
    states_block, gram_sum = teacher_block(place, kept, arrived, columns, teacher_final_gain)
    bits = dp_count.bit_length() - 1
    for bit in range(bits):
        gram_kept = gram_sum
        gram_arrived = swap(gram_sum, "dp", bit)
        gram_sum = gram_kept + gram_arrived

    grads, acts, states = zip(first, second)
    pooled_act = jnp.concatenate(acts)[:, 0].astype(bf16)
    pooled_x = jnp.concatenate(states)[:, 0]
    emb_sum = jnp.dot(pooled_act, student_w_out, preferred_element_type=f32)
    for bit in range(section_count.bit_length() - 1):
        emb_sum = emb_sum + swap(emb_sum, "section", bit)
    far_first = tuple(reversed(range(bits)))
    every_raw = (pooled_x + emb_sum)[None]
    for bit in far_first:
        every_raw = jnp.concatenate([every_raw, swap(every_raw, "dp", bit)])
    unit, norms, student_logits = embed(place, every_raw, far_first)
    orders = (tuple(range(bits)), (1, 0) + tuple(range(2, bits)))
    loss, every_low, scale, *sent = contrast(
        place,
        lengths,
        gram_kept,
        gram_arrived,
        student_logits,
        unit,
        norms,
        student_w_out,
        grads,
        orders,
        dp_count,
    )

    kept = weigh(place, scale, grads, orders, dp_count, sent)
    sides = []
    for side in range(2):
        sides.append(halving(sent[side], kept[side], orders[side], "dp"))
    grad_w_in = jnp.concatenate(sides, axis=1)
    pooled = pooled_act.reshape(local_docs, dp_count, -1).transpose(1, 0, 2).astype(f32)
    states_block = states_block.reshape(dp_count, local_docs, col_width)
    last = exchange(jnp.concatenate([states_block, pooled], axis=2), "dp")
    per_section = dp_count // section_count
    own_blocks = lax.dynamic_slice_in_dim(last, section_index * per_section, per_section, 0)
    own_blocks = own_blocks[:, :, :col_width].transpose(1, 0, 2)
    teacher_states = own_blocks.reshape(local_docs, per_section * col_width)
    pooled_columns = last[:, :, col_width:].reshape(total_docs, -1).astype(bf16)
    grad_w_out = lax.dot_general(
        pooled_columns, every_low, (((0,), (0,)), ((), ())), preferred_element_type=f32
    )
    return (loss[0, 0], grad_w_in, grad_w_out, teacher_states)


def solution(mesh):
    placed = (
        P("dp", None, None),
        P("dp"),
        P(),
        P(None, "section"),
        P("section", None),
        P("dp", None),
        P(),
        P(None, "dp", "section"),
        P("section", "dp"),
        P(),
    )

    return jax.shard_map(
        on_device,
        mesh=mesh,
        in_specs=placed,
        out_specs=(P(), P("dp", "section"), P(("section", "dp"), None), P("dp", "section")),
        check_vma=False,
    )
```

```python
import functools

import jax
import jax.numpy as jnp
from jax import lax
from jax.experimental import pallas as pl
from jax.experimental.pallas import tpu as pltpu
from jax.sharding import PartitionSpec as P


student_softness = 0.05
teacher_softness = 0.02
f32 = jnp.float32
bf16 = jnp.bfloat16
highest = lax.Precision.HIGHEST


def exchange(blocks, axis):
    return lax.all_to_all(blocks, axis, 0, 0, tiled=True)


def swap(value, axis, bit):
    members = lax.axis_size(axis)
    return lax.ppermute(value, axis, [(i, i ^ (1 << bit)) for i in range(members)])


def student_doc(rows, length, states, gain, w_in, grad, pool_act, pool_x):
    low = states[0, :rows, :]
    values = low.astype(f32)
    center = values - jnp.mean(values, -1, keepdims=True)
    spread = jnp.mean(center * center, -1, keepdims=True)
    real = lax.broadcasted_iota(jnp.int32, (rows, 1), 0) < length
    inverse = jnp.where(real, lax.rsqrt(spread + 1e-05), 0.0)
    tokens = (center * inverse * gain[...]).astype(bf16)
    real = lax.broadcasted_iota(jnp.int32, (8, rows), 1) < length
    sums = jnp.dot(real.astype(bf16), low, preferred_element_type=f32)
    count = length.astype(f32)
    pool_x[0] = sums[:1] / count
    pre_act = jnp.dot(tokens, w_in[...], preferred_element_type=f32)
    half_erf = 0.5 * (1.0 + lax.erf(pre_act * 0.7071067811865476))
    act = (pre_act * half_erf).astype(bf16)
    bell = jnp.exp(-0.5 * pre_act * pre_act)
    slope = (half_erf + pre_act * bell * 0.3989422804014327).astype(bf16)
    pool_act[0] = jnp.sum(act.astype(f32), 0, keepdims=True) / count
    product = lax.dot_general(
        tokens, slope, (((0,), (0,)), ((), ())), preferred_element_type=f32
    )
    half = grad.shape[3]
    for side in range(grad.shape[1]):
        grad[0, side] = product[:, side * half : (side + 1) * half].astype(bf16)


def student_kernel(first_doc, lens, states, gain, w_in, after, grad, pool_act, pool_x):
    length = lens[first_doc + pl.program_id(0)]
    seq_len = states.shape[1]
    refs = (states, gain, w_in, grad, pool_act, pool_x)
    lines = 128 if seq_len % 128 == 0 else seq_len
    for rows in range(lines, seq_len + 1, lines):

        @pl.when((length > rows - lines) & (length <= rows))
        def _(rows=rows):
            student_doc(rows, length, *refs)


def student_part(lengths, states, gain, w_in, after, first_doc, docs):
    seq_len, width = states.shape[1:]
    hidden = w_in.shape[1]
    return pl.pallas_call(
        functools.partial(student_kernel, first_doc),
        grid_spec=pltpu.PrefetchScalarGridSpec(
            num_scalar_prefetch=1,
            grid=(docs,),
            in_specs=[
                pl.BlockSpec((1, seq_len, width), lambda i, n: (first_doc + i, 0, 0)),
                pl.BlockSpec((1, width), lambda i, n: (0, 0)),
                pl.BlockSpec((width, hidden), lambda i, n: (0, 0)),
                pl.BlockSpec(memory_space=pl.ANY),
            ],
            out_specs=[
                pl.BlockSpec((1, 2, width, hidden // 2), lambda i, n: (i, 0, 0, 0)),
                pl.BlockSpec((1, 1, hidden), lambda i, n: (i, 0, 0)),
                pl.BlockSpec((1, 1, width), lambda i, n: (i, 0, 0)),
            ],
        ),
        out_shape=[
            jax.ShapeDtypeStruct((docs, 2, width, hidden // 2), bf16),
            jax.ShapeDtypeStruct((docs, 1, hidden), f32),
            jax.ShapeDtypeStruct((docs, 1, width), f32),
        ],
        compiler_params=pltpu.CompilerParams(
            dimension_semantics=("arbitrary",), vmem_limit_bytes=59 << 20
        ),
        cost_estimate=pl.CostEstimate(
            flops=3 * docs * seq_len * width * hidden,
            bytes_accessed=docs * width * (seq_len + hidden) * 2,
            transcendentals=docs * seq_len * hidden,
        ),
        name="student",
    )(lengths, states, gain.reshape(1, width), w_in, after)


def gate_up_kernel(block, place, columns, gain, weights, parts, held, arrived):
    hidden = weights.shape[2]
    copies = []
    for i in range(hidden // block):
        here = pl.ds(i * block, block)
        copies.append(
            pltpu.make_async_copy(weights.at[:, :, here], held.at[:, :, here], arrived.at[i])
        )
        copies[-1].start()
    depth = columns.shape[1]
    factors = gain[:, pl.ds(pl.multiple_of(place[0] * depth, depth), depth)]
    scaled = (columns[...].astype(f32) * factors).astype(bf16)
    for i, copy in enumerate(copies):
        copy.wait()
        for side in range(2):
            part = jnp.dot(
                scaled, held[side, :, i * block : (i + 1) * block], preferred_element_type=f32
            )
            first = (2 * i + side) * block
            parts[:, first : first + block] = part.astype(bf16)


def gate_up(place, columns, gain, weights, block):
    hidden = weights.shape[2]
    vmem = pl.BlockSpec(memory_space=pltpu.VMEM)
    return pl.pallas_call(
        functools.partial(gate_up_kernel, block),
        in_specs=[
            pl.BlockSpec(memory_space=pltpu.SMEM),
            vmem,
            vmem,
            pl.BlockSpec(memory_space=pltpu.HBM),
        ],
        out_specs=vmem,
        out_shape=jax.ShapeDtypeStruct((columns.shape[0], 2 * hidden), bf16),
        scratch_shapes=[
            pltpu.VMEM(weights.shape, bf16),
            pltpu.SemaphoreType.DMA((hidden // block,)),
        ],
        compiler_params=pltpu.CompilerParams(vmem_limit_bytes=59 << 20),
        name="gate_up",
    )(place, columns, gain.reshape(1, -1), weights)


def hidden_kernel(block, parts, rows, hidden):
    row = rows[...].astype(f32)
    inverse = lax.rsqrt(jnp.mean(row * row, -1, keepdims=True) + 1e-06)
    for first in range(0, hidden.shape[2], block):
        both = jnp.sum(parts[:, :, 2 * first : 2 * (first + block)].astype(f32), 0) * inverse
        gate, upper = both[:, :block], both[:, block:]
        value = (gate / (1.0 + jnp.exp(-gate)) * upper).astype(bf16)
        for copy in range(hidden.shape[0]):
            hidden[copy, :, first : first + block] = value


def hidden_units(parts, rows, block):
    members, docs, both = parts.shape
    return pl.pallas_call(
        functools.partial(hidden_kernel, block),
        out_shape=jax.ShapeDtypeStruct((members, docs, both // 2), bf16),
        compiler_params=pltpu.CompilerParams(vmem_limit_bytes=12 << 20),
        name="hidden",
    )(parts, rows)


def down_kernel(hidden, weights, out):
    out[...] = jnp.dot(hidden[...], weights[...], preferred_element_type=f32)


def down(hidden, weights):
    return pl.pallas_call(
        down_kernel,
        out_shape=jax.ShapeDtypeStruct((hidden.shape[0], weights.shape[1]), f32),
        compiler_params=pltpu.CompilerParams(vmem_limit_bytes=12 << 20),
        name="down",
    )(hidden, weights)


def states_kernel(place, kept, arrived, columns, gain, states, gram):
    value = columns[...].astype(f32) + (kept[...].astype(f32) + arrived[...].astype(f32))
    states[...] = value
    width = value.shape[1]
    scaled = value * gain[:, pl.ds(pl.multiple_of(place[0] * width, width), width)]
    product = lax.dot_general(
        scaled, scaled, (((1,), (1,)), ((), ())), precision=highest, preferred_element_type=f32
    )
    rows = gram.shape[0]
    packed = [product[i : i + rows] for i in range(0, product.shape[0], rows)]
    gram[...] = packed[0] if len(packed) == 1 else jnp.concatenate(packed, axis=1)


def packed_rows(docs):
    return docs * docs // 128 if docs < 128 and 128 % docs == 0 else docs


def teacher_block(place, kept, arrived, columns, gain):
    docs, width = columns.shape
    rows = packed_rows(docs)
    vmem = pl.BlockSpec(memory_space=pltpu.VMEM)
    return pl.pallas_call(
        states_kernel,
        in_specs=[pl.BlockSpec(memory_space=pltpu.SMEM)] + [vmem] * 4,
        out_specs=[vmem] * 2,
        out_shape=[
            jax.ShapeDtypeStruct((docs, width), f32),
            jax.ShapeDtypeStruct((rows, docs * docs // rows), f32),
        ],
        compiler_params=pltpu.CompilerParams(vmem_limit_bytes=8 << 20),
        name="teacher_block",
    )(place, kept, arrived, columns, gain.reshape(1, -1))


def embed_kernel(order, place, blocks, unit, norms, logits, raw):
    docs = blocks.shape[1]
    for i in range(blocks.shape[0]):
        member = place[0] ^ sum(((i >> k) & 1) << bit for k, bit in enumerate(order))
        raw[pl.ds(pl.multiple_of(member * docs, docs), docs), :] = blocks[i]
    value = raw[...]
    size = jnp.sqrt(jnp.sum(value * value, -1, keepdims=True) + 1e-06)
    units = value / size
    norms[...] = size
    unit[...] = units
    logits[...] = (
        lax.dot_general(
            units, units, (((1,), (1,)), ((), ())), precision=highest, preferred_element_type=f32
        )
        / student_softness
    )


def embed(place, blocks, order):
    members, each, width = blocks.shape
    docs = members * each
    vmem = pl.BlockSpec(memory_space=pltpu.VMEM)
    return pl.pallas_call(
        functools.partial(embed_kernel, order),
        in_specs=[pl.BlockSpec(memory_space=pltpu.SMEM), vmem],
        out_specs=[vmem] * 3,
        out_shape=[
            jax.ShapeDtypeStruct((docs, width), f32),
            jax.ShapeDtypeStruct((docs, 1), f32),
            jax.ShapeDtypeStruct((docs, docs), f32),
        ],
        scratch_shapes=[pltpu.VMEM((docs, width), f32)],
        compiler_params=pltpu.CompilerParams(vmem_limit_bytes=8 << 20),
        name="embed",
    )(place, blocks)


def relative(order, step):
    return sum(((step >> (len(order) - 1 - k)) & 1) << bit for k, bit in enumerate(order))


def fetch(plan, place, grads, held, arrived):
    orders, first = plan
    rows = held[0].shape[-2]
    copies = []
    for side, order in enumerate(orders):
        for i in range(held[0].shape[1]):
            member = place[0] ^ relative(order, first + i)
            here = pl.ds(pl.multiple_of(member * rows, rows), rows)
            group = [
                pltpu.make_async_copy(
                    grad.at[:, side, here, :],
                    buffer.at[side, i],
                    arrived.at[part, side, i],
                )
                for part, (grad, buffer) in enumerate(zip(grads, held))
            ]
            for copy in group:
                copy.start()
            copies.append((side, i, group))
    return copies


def weigh_fetched(copies, scale, held, outs):
    half, rows = held[0].shape[-1], held[0].shape[-2]
    lines = 16
    for side, i, group in copies:
        for copy in group:
            copy.wait()
        factors = scale[:, side * half : (side + 1) * half]

        def step(line, carry, side=side, i=i, factors=factors):
            here = pl.ds(pl.multiple_of(line * lines, lines), lines)
            total, doc = None, 0
            for buffer in held:
                for j in range(buffer.shape[2]):
                    term = buffer[side, i, j, here, :].astype(f32) * factors[doc : doc + 1]
                    total = term if total is None else total + term
                    doc += 1
            outs[side][i, here, :] = total.astype(bf16)
            return carry

        lax.fori_loop(0, rows // lines, step, 0)


def block_shapes(grads, members):
    width, half = grads[0].shape[2:]
    rows, count = width // members, members // 2
    buffers = [pltpu.VMEM((2, count, grad.shape[0], rows, half), bf16) for grad in grads]
    arrived = pltpu.SemaphoreType.DMA((len(grads), 2, count))
    return buffers, arrived, [jax.ShapeDtypeStruct((count, rows, half), bf16)] * 2


def contrast_kernel(plan, place, lens, gram_kept, gram_arrived, logits, unit, norms, w_out, *refs):
    parts = (len(refs) - 9) // 2
    grads, refs = refs[:parts], refs[parts:]
    (loss, low, scale), outs, (raw, weights), refs = refs[:3], refs[3:5], refs[5:7], refs[7:]
    held, (weights_here, arrived) = refs[:-2], refs[-2:]
    copy = pltpu.make_async_copy(w_out, weights, weights_here)
    copy.start()
    copies = fetch(plan, place, grads, held, arrived)
    gram = gram_kept[...] + gram_arrived[...]
    docs = logits.shape[0]
    if gram.shape[1] != docs:
        gram = jnp.concatenate(
            [gram[:, i : i + docs] for i in range(0, gram.shape[1], docs)], axis=0
        )
    row = lax.broadcasted_iota(jnp.int32, (docs, docs), 0)
    col = lax.broadcasted_iota(jnp.int32, (docs, docs), 1)
    keep = row != col
    partner = (row + 1 - 2 * (row % 2)) == col
    own = jnp.where(keep, 0.0, gram)
    sizes_down = jnp.sqrt(jnp.sum(own, 1, keepdims=True) + 1e-06)
    sizes_along = jnp.sqrt(jnp.sum(own, 0, keepdims=True) + 1e-06)
    t_logits = gram / (sizes_down * sizes_along) / teacher_softness
    s_logits = logits[...]
    t_exp = jnp.where(keep, jnp.exp(t_logits), 0.0)
    s_exp = jnp.where(keep, jnp.exp(s_logits), 0.0)
    t_down = jnp.sum(t_exp, 1, keepdims=True)
    s_down = jnp.sum(s_exp, 1, keepdims=True)
    t_along = jnp.sum(t_exp, 0, keepdims=True)
    s_along = jnp.sum(s_exp, 0, keepdims=True)
    s_log = s_logits - jnp.log(s_down)
    t_log = t_logits - jnp.log(t_down)
    terms = jnp.where(partner, -s_log, 0.0)
    terms = terms + jnp.where(keep, t_exp / t_down * (t_log - s_log), 0.0)
    loss[...] = jnp.sum(jnp.sum(terms, 1, keepdims=True), 0, keepdims=True)
    both = 2.0 * (s_exp / s_down + s_exp / s_along) - (t_exp / t_down + t_exp / t_along)
    both = both - jnp.where(partner, 2.0, 0.0)
    units = unit[...]
    unit_grad = (
        jnp.dot(both, units, precision=highest, preferred_element_type=f32) / student_softness
    )
    along = jnp.sum(units * unit_grad, -1, keepdims=True)
    raw_low = ((unit_grad - units * along) / norms[...]).astype(bf16)
    low[...] = raw_low
    raw[...] = raw_low.astype(f32)
    mine = raw[pl.ds(pl.multiple_of(place[0] * scale.shape[0], scale.shape[0]), scale.shape[0]), :]
    copy.wait()
    pool_grad = lax.dot_general(
        mine.astype(bf16), weights[...], (((1,), (1,)), ((), ())), preferred_element_type=f32
    )
    for doc in range(scale.shape[0]):
        scale[doc : doc + 1, :] = pool_grad[doc : doc + 1, :] / lens[doc].astype(f32)
    weigh_fetched(copies, scale, held, outs)


def contrast(place, lengths, gram_kept, gram_arrived, logits, unit, norms, w_out, grads, orders, members):
    total_docs, width = unit.shape
    local_docs, hidden = lengths.shape[0], w_out.shape[0]
    buffers, arrived, sums = block_shapes(grads, members)
    vmem, smem = pl.BlockSpec(memory_space=pltpu.VMEM), pl.BlockSpec(memory_space=pltpu.SMEM)
    hbm = pl.BlockSpec(memory_space=pltpu.HBM)
    return pl.pallas_call(
        functools.partial(contrast_kernel, (orders, members // 2)),
        in_specs=[smem] * 2 + [vmem] * 5 + [hbm] * (1 + len(grads)),
        out_specs=[vmem] * 5,
        out_shape=[
            jax.ShapeDtypeStruct((1, 1), f32),
            jax.ShapeDtypeStruct((total_docs, width), bf16),
            jax.ShapeDtypeStruct((local_docs, hidden), f32),
        ]
        + sums,
        scratch_shapes=[pltpu.VMEM((total_docs, width), f32), pltpu.VMEM(w_out.shape, bf16)]
        + buffers
        + [pltpu.SemaphoreType.DMA, arrived],
        compiler_params=pltpu.CompilerParams(vmem_limit_bytes=50 << 20),
        name="contrast",
    )(place, lengths, gram_kept, gram_arrived, logits, unit, norms, w_out, *grads)


def weigh_kernel(plan, parts, place, scale, *refs):
    grads, outs, held, arrived = refs[:parts], refs[-3 - parts : -1 - parts], refs[-1 - parts : -1], refs[-1]
    weigh_fetched(fetch(plan, place, grads, held, arrived), scale, held, outs)


def weigh(place, scale, grads, orders, members, after):
    buffers, arrived, sums = block_shapes(grads, members)
    vmem, smem = pl.BlockSpec(memory_space=pltpu.VMEM), pl.BlockSpec(memory_space=pltpu.SMEM)
    hbm, kept = pl.BlockSpec(memory_space=pltpu.HBM), pl.BlockSpec(memory_space=pl.ANY)
    return pl.pallas_call(
        functools.partial(weigh_kernel, (orders, 0), len(grads)),
        in_specs=[smem, vmem] + [hbm] * len(grads) + [kept] * len(after),
        out_specs=[vmem] * 2,
        out_shape=sums,
        scratch_shapes=buffers + [arrived],
        compiler_params=pltpu.CompilerParams(vmem_limit_bytes=50 << 20),
        name="weigh",
    )(place, scale, *grads, *after)


def halving(sent, kept, order, axis):
    for bit in order:
        arrived = swap(sent, axis, bit)
        rest = kept.shape[0] // 2
        if rest:
            sent = (kept[rest:].astype(f32) + arrived[rest:].astype(f32)).astype(bf16)
            kept = (kept[:rest].astype(f32) + arrived[:rest].astype(f32)).astype(bf16)
    return kept[0].astype(f32) + arrived[0].astype(f32)


def on_device(
    student_states,
    lengths,
    student_ln_gain,
    student_w_in,
    student_w_out,
    teacher_rows,
    teacher_mlp_gain,
    teacher_gate_up,
    teacher_down,
    teacher_final_gain,
):
    dp_count = lax.axis_size("dp")
    section_count = lax.axis_size("section")
    dp_index = lax.axis_index("dp")
    section_index = lax.axis_index("section")
    local_docs = teacher_rows.shape[0]
    total_docs = local_docs * dp_count
    col_width = teacher_gate_up.shape[1]
    hidden_width = teacher_gate_up.shape[2]
    place = dp_index.astype(jnp.int32).reshape(1)
    block = hidden_width // 6 if hidden_width % 768 == 0 else hidden_width
    student = functools.partial(
        student_part, lengths, student_states, student_ln_gain, student_w_in
    )
    early = local_docs // 4

    blocks = teacher_rows.reshape(local_docs, dp_count, col_width).transpose(1, 0, 2)
    columns = exchange(blocks, "dp").reshape(total_docs, col_width)
    first = student(teacher_rows, 0, early)
    parts = gate_up(place, columns, teacher_mlp_gain, teacher_gate_up, block)
    parts = parts.reshape(dp_count, local_docs, 2 * hidden_width)
    second = student(parts, early, local_docs - early)
    parts = exchange(parts, "dp")
    hidden = hidden_units(parts, teacher_rows, block)
    every_hidden = exchange(hidden, "dp").reshape(total_docs, hidden_width)
    out = down(every_hidden, teacher_down)
    for bit in range(section_count.bit_length() - 1):
        kept = out if bit == 0 else out.astype(bf16)
        arrived = swap(kept, "section", bit)
        out = kept.astype(f32) + arrived.astype(f32)
    states_block, gram_sum = teacher_block(place, kept, arrived, columns, teacher_final_gain)
    bits = dp_count.bit_length() - 1
    for bit in range(bits):
        gram_kept = gram_sum
        gram_arrived = swap(gram_sum, "dp", bit)
        gram_sum = gram_kept + gram_arrived

    grads, acts, states = zip(first, second)
    pooled_act = jnp.concatenate(acts)[:, 0].astype(bf16)
    pooled_x = jnp.concatenate(states)[:, 0]
    emb_sum = jnp.dot(pooled_act, student_w_out, preferred_element_type=f32)
    for bit in range(section_count.bit_length() - 1):
        emb_sum = emb_sum + swap(emb_sum, "section", bit)
    far_first = tuple(reversed(range(bits)))
    every_raw = (pooled_x + emb_sum)[None]
    for bit in far_first:
        every_raw = jnp.concatenate([every_raw, swap(every_raw, "dp", bit)])
    unit, norms, student_logits = embed(place, every_raw, far_first)
    orders = (tuple(range(bits)), (1, 0) + tuple(range(2, bits)))
    loss, every_low, scale, *sent = contrast(
        place,
        lengths,
        gram_kept,
        gram_arrived,
        student_logits,
        unit,
        norms,
        student_w_out,
        grads,
        orders,
        dp_count,
    )

    kept = weigh(place, scale, grads, orders, dp_count, sent)
    sides = []
    for side in range(2):
        sides.append(halving(sent[side], kept[side], orders[side], "dp"))
    grad_w_in = jnp.concatenate(sides, axis=1)
    pooled = pooled_act.reshape(local_docs, dp_count, -1).transpose(1, 0, 2).astype(f32)
    states_block = states_block.reshape(dp_count, local_docs, col_width)
    last = exchange(jnp.concatenate([states_block, pooled], axis=2), "dp")
    per_section = dp_count // section_count
    own_blocks = lax.dynamic_slice_in_dim(last, section_index * per_section, per_section, 0)
    own_blocks = own_blocks[:, :, :col_width].transpose(1, 0, 2)
    teacher_states = own_blocks.reshape(local_docs, per_section * col_width)
    pooled_columns = last[:, :, col_width:].reshape(total_docs, -1).astype(bf16)
    grad_w_out = lax.dot_general(
        pooled_columns, every_low, (((0,), (0,)), ((), ())), preferred_element_type=f32
    )
    return (loss[0, 0], grad_w_in, grad_w_out, teacher_states)


def solution(mesh):
    placed = (
        P("dp", None, None),
        P("dp"),
        P(),
        P(None, "section"),
        P("section", None),
        P("dp", None),
        P(),
        P(None, "dp", "section"),
        P("section", "dp"),
        P(),
    )

    return jax.shard_map(
        on_device,
        mesh=mesh,
        in_specs=placed,
        out_specs=(P(), P("dp", "section"), P(("section", "dp"), None), P("dp", "section")),
        check_vma=False,
    )
```

```python
import functools

import jax
import jax.numpy as jnp
from jax import lax
from jax.experimental import pallas as pl
from jax.experimental.pallas import tpu as pltpu
from jax.sharding import PartitionSpec as P


student_softness = 0.05
teacher_softness = 0.02
f32 = jnp.float32
bf16 = jnp.bfloat16
highest = lax.Precision.HIGHEST


def exchange(blocks, axis):
    return lax.all_to_all(blocks, axis, 0, 0, tiled=True)


def swap(value, axis, bit):
    members = lax.axis_size(axis)
    return lax.ppermute(value, axis, [(i, i ^ (1 << bit)) for i in range(members)])


def student_doc(rows, length, states, gain, w_in, grad, pool_act, pool_x):
    low = states[0, :rows, :]
    values = low.astype(f32)
    center = values - jnp.mean(values, -1, keepdims=True)
    spread = jnp.mean(center * center, -1, keepdims=True)
    real = lax.broadcasted_iota(jnp.int32, (rows, 1), 0) < length
    inverse = jnp.where(real, lax.rsqrt(spread + 1e-05), 0.0)
    tokens = (center * inverse * gain[...]).astype(bf16)
    real = lax.broadcasted_iota(jnp.int32, (8, rows), 1) < length
    sums = jnp.dot(real.astype(bf16), low, preferred_element_type=f32)
    count = length.astype(f32)
    pool_x[0] = sums[:1] / count
    pre_act = jnp.dot(tokens, w_in[...], preferred_element_type=f32)
    half_erf = 0.5 * (1.0 + lax.erf(pre_act * 0.7071067811865476))
    act = (pre_act * half_erf).astype(bf16)
    bell = jnp.exp(-0.5 * pre_act * pre_act)
    slope = (half_erf + pre_act * bell * 0.3989422804014327).astype(bf16)
    pool_act[0] = jnp.sum(act.astype(f32), 0, keepdims=True) / count
    product = lax.dot_general(
        tokens, slope, (((0,), (0,)), ((), ())), preferred_element_type=f32
    )
    half = grad.shape[3]
    for side in range(grad.shape[1]):
        grad[0, side] = product[:, side * half : (side + 1) * half].astype(bf16)


def student_kernel(first_doc, lens, states, gain, w_in, after, grad, pool_act, pool_x):
    length = lens[first_doc + pl.program_id(0)]
    seq_len = states.shape[1]
    refs = (states, gain, w_in, grad, pool_act, pool_x)
    lines = 128 if seq_len % 128 == 0 else seq_len
    for rows in range(lines, seq_len + 1, lines):

        @pl.when((length > rows - lines) & (length <= rows))
        def _(rows=rows):
            student_doc(rows, length, *refs)


def student_part(lengths, states, gain, w_in, after, first_doc, docs):
    seq_len, width = states.shape[1:]
    hidden = w_in.shape[1]
    return pl.pallas_call(
        functools.partial(student_kernel, first_doc),
        grid_spec=pltpu.PrefetchScalarGridSpec(
            num_scalar_prefetch=1,
            grid=(docs,),
            in_specs=[
                pl.BlockSpec((1, seq_len, width), lambda i, n: (first_doc + i, 0, 0)),
                pl.BlockSpec((1, width), lambda i, n: (0, 0)),
                pl.BlockSpec((width, hidden), lambda i, n: (0, 0)),
                pl.BlockSpec(memory_space=pl.ANY),
            ],
            out_specs=[
                pl.BlockSpec((1, 2, width, hidden // 2), lambda i, n: (i, 0, 0, 0)),
                pl.BlockSpec((1, 1, hidden), lambda i, n: (i, 0, 0)),
                pl.BlockSpec((1, 1, width), lambda i, n: (i, 0, 0)),
            ],
        ),
        out_shape=[
            jax.ShapeDtypeStruct((docs, 2, width, hidden // 2), bf16),
            jax.ShapeDtypeStruct((docs, 1, hidden), f32),
            jax.ShapeDtypeStruct((docs, 1, width), f32),
        ],
        compiler_params=pltpu.CompilerParams(
            dimension_semantics=("arbitrary",), vmem_limit_bytes=59 << 20
        ),
        cost_estimate=pl.CostEstimate(
            flops=3 * docs * seq_len * width * hidden,
            bytes_accessed=docs * width * (seq_len + hidden) * 2,
            transcendentals=docs * seq_len * hidden,
        ),
        name="student",
    )(lengths, states, gain.reshape(1, width), w_in, after)


def gate_up_kernel(block, place, columns, gain, weights, parts, held, arrived):
    hidden = weights.shape[2]
    copies = []
    for i in range(hidden // block):
        here = pl.ds(i * block, block)
        copies.append(
            pltpu.make_async_copy(weights.at[:, :, here], held.at[:, :, here], arrived.at[i])
        )
        copies[-1].start()
    depth = columns.shape[1]
    factors = gain[:, pl.ds(pl.multiple_of(place[0] * depth, depth), depth)]
    scaled = (columns[...].astype(f32) * factors).astype(bf16)
    for i, copy in enumerate(copies):
        copy.wait()
        for side in range(2):
            part = jnp.dot(
                scaled, held[side, :, i * block : (i + 1) * block], preferred_element_type=f32
            )
            first = (2 * i + side) * block
            parts[:, first : first + block] = part.astype(bf16)


def gate_up(place, columns, gain, weights, block):
    hidden = weights.shape[2]
    vmem = pl.BlockSpec(memory_space=pltpu.VMEM)
    return pl.pallas_call(
        functools.partial(gate_up_kernel, block),
        in_specs=[
            pl.BlockSpec(memory_space=pltpu.SMEM),
            vmem,
            vmem,
            pl.BlockSpec(memory_space=pltpu.HBM),
        ],
        out_specs=vmem,
        out_shape=jax.ShapeDtypeStruct((columns.shape[0], 2 * hidden), bf16),
        scratch_shapes=[
            pltpu.VMEM(weights.shape, bf16),
            pltpu.SemaphoreType.DMA((hidden // block,)),
        ],
        compiler_params=pltpu.CompilerParams(vmem_limit_bytes=59 << 20),
        name="gate_up",
    )(place, columns, gain.reshape(1, -1), weights)


def hidden_kernel(block, parts, rows, hidden):
    row = rows[...].astype(f32)
    inverse = lax.rsqrt(jnp.mean(row * row, -1, keepdims=True) + 1e-06)
    for first in range(0, hidden.shape[2], block):
        both = jnp.sum(parts[:, :, 2 * first : 2 * (first + block)].astype(f32), 0) * inverse
        gate, upper = both[:, :block], both[:, block:]
        value = (gate / (1.0 + jnp.exp(-gate)) * upper).astype(bf16)
        for copy in range(hidden.shape[0]):
            hidden[copy, :, first : first + block] = value


def hidden_units(parts, rows, block):
    members, docs, both = parts.shape
    return pl.pallas_call(
        functools.partial(hidden_kernel, block),
        out_shape=jax.ShapeDtypeStruct((members, docs, both // 2), bf16),
        compiler_params=pltpu.CompilerParams(vmem_limit_bytes=12 << 20),
        name="hidden",
    )(parts, rows)


def down_kernel(hidden, weights, out):
    out[...] = jnp.dot(hidden[...], weights[...], preferred_element_type=f32)


def down(hidden, weights):
    return pl.pallas_call(
        down_kernel,
        out_shape=jax.ShapeDtypeStruct((hidden.shape[0], weights.shape[1]), f32),
        compiler_params=pltpu.CompilerParams(vmem_limit_bytes=12 << 20),
        name="down",
    )(hidden, weights)


def states_kernel(place, kept, arrived, columns, gain, states, gram):
    value = columns[...].astype(f32) + (kept[...].astype(f32) + arrived[...].astype(f32))
    states[...] = value
    width = value.shape[1]
    scaled = value * gain[:, pl.ds(pl.multiple_of(place[0] * width, width), width)]
    product = lax.dot_general(
        scaled, scaled, (((1,), (1,)), ((), ())), precision=highest, preferred_element_type=f32
    )
    rows = gram.shape[0]
    packed = [product[i : i + rows] for i in range(0, product.shape[0], rows)]
    gram[...] = packed[0] if len(packed) == 1 else jnp.concatenate(packed, axis=1)


def packed_rows(docs):
    return docs * docs // 128 if docs < 128 and 128 % docs == 0 else docs


def teacher_block(place, kept, arrived, columns, gain):
    docs, width = columns.shape
    rows = packed_rows(docs)
    vmem = pl.BlockSpec(memory_space=pltpu.VMEM)
    return pl.pallas_call(
        states_kernel,
        in_specs=[pl.BlockSpec(memory_space=pltpu.SMEM)] + [vmem] * 4,
        out_specs=[vmem] * 2,
        out_shape=[
            jax.ShapeDtypeStruct((docs, width), f32),
            jax.ShapeDtypeStruct((rows, docs * docs // rows), f32),
        ],
        compiler_params=pltpu.CompilerParams(vmem_limit_bytes=8 << 20),
        name="teacher_block",
    )(place, kept, arrived, columns, gain.reshape(1, -1))


def embed_kernel(order, place, blocks, unit, norms, logits, raw):
    docs = blocks.shape[1]
    for i in range(blocks.shape[0]):
        member = place[0] ^ sum(((i >> k) & 1) << bit for k, bit in enumerate(order))
        raw[pl.ds(pl.multiple_of(member * docs, docs), docs), :] = blocks[i]
    value = raw[...]
    size = jnp.sqrt(jnp.sum(value * value, -1, keepdims=True) + 1e-06)
    units = value / size
    norms[...] = size
    unit[...] = units
    logits[...] = (
        lax.dot_general(
            units, units, (((1,), (1,)), ((), ())), precision=highest, preferred_element_type=f32
        )
        / student_softness
    )


def embed(place, blocks, order):
    members, each, width = blocks.shape
    docs = members * each
    vmem = pl.BlockSpec(memory_space=pltpu.VMEM)
    return pl.pallas_call(
        functools.partial(embed_kernel, order),
        in_specs=[pl.BlockSpec(memory_space=pltpu.SMEM), vmem],
        out_specs=[vmem] * 3,
        out_shape=[
            jax.ShapeDtypeStruct((docs, width), f32),
            jax.ShapeDtypeStruct((docs, 1), f32),
            jax.ShapeDtypeStruct((docs, docs), f32),
        ],
        scratch_shapes=[pltpu.VMEM((docs, width), f32)],
        compiler_params=pltpu.CompilerParams(vmem_limit_bytes=8 << 20),
        name="embed",
    )(place, blocks)


def relative(order, step):
    return sum(((step >> (len(order) - 1 - k)) & 1) << bit for k, bit in enumerate(order))


def fetch(plan, place, grads, held, arrived):
    orders, first = plan
    rows = held[0].shape[-2]
    copies = []
    for side, order in enumerate(orders):
        for i in range(held[0].shape[1]):
            member = place[0] ^ relative(order, first + i)
            here = pl.ds(pl.multiple_of(member * rows, rows), rows)
            group = [
                pltpu.make_async_copy(
                    grad.at[:, side, here, :],
                    buffer.at[side, i],
                    arrived.at[part, side, i],
                )
                for part, (grad, buffer) in enumerate(zip(grads, held))
            ]
            for copy in group:
                copy.start()
            copies.append((side, i, group))
    return copies


def weigh_fetched(copies, scale, held, outs):
    half, rows = held[0].shape[-1], held[0].shape[-2]
    lines = 16
    for side, i, group in copies:
        for copy in group:
            copy.wait()
        factors = scale[:, side * half : (side + 1) * half]

        def step(line, carry, side=side, i=i, factors=factors):
            here = pl.ds(pl.multiple_of(line * lines, lines), lines)
            total, doc = None, 0
            for buffer in held:
                for j in range(buffer.shape[2]):
                    term = buffer[side, i, j, here, :].astype(f32) * factors[doc : doc + 1]
                    total = term if total is None else total + term
                    doc += 1
            outs[side][i, here, :] = total.astype(bf16)
            return carry

        lax.fori_loop(0, rows // lines, step, 0)


def block_shapes(grads, members):
    width, half = grads[0].shape[2:]
    rows, count = width // members, members // 2
    buffers = [pltpu.VMEM((2, count, grad.shape[0], rows, half), bf16) for grad in grads]
    arrived = pltpu.SemaphoreType.DMA((len(grads), 2, count))
    return buffers, arrived, [jax.ShapeDtypeStruct((count, rows, half), bf16)] * 2


def contrast_kernel(plan, place, lens, gram_kept, gram_arrived, logits, unit, norms, w_out, *refs):
    parts = (len(refs) - 9) // 2
    grads, refs = refs[:parts], refs[parts:]
    (loss, low, scale), outs, (raw, weights), refs = refs[:3], refs[3:5], refs[5:7], refs[7:]
    held, (weights_here, arrived) = refs[:-2], refs[-2:]
    copy = pltpu.make_async_copy(w_out, weights, weights_here)
    copy.start()
    copies = fetch(plan, place, grads, held, arrived)
    gram = gram_kept[...] + gram_arrived[...]
    docs = logits.shape[0]
    if gram.shape[1] != docs:
        gram = jnp.concatenate(
            [gram[:, i : i + docs] for i in range(0, gram.shape[1], docs)], axis=0
        )
    row = lax.broadcasted_iota(jnp.int32, (docs, docs), 0)
    col = lax.broadcasted_iota(jnp.int32, (docs, docs), 1)
    keep = row != col
    partner = (row + 1 - 2 * (row % 2)) == col
    own = jnp.where(keep, 0.0, gram)
    sizes_down = jnp.sqrt(jnp.sum(own, 1, keepdims=True) + 1e-06)
    sizes_along = jnp.sqrt(jnp.sum(own, 0, keepdims=True) + 1e-06)
    t_logits = gram / (sizes_down * sizes_along) / teacher_softness
    s_logits = logits[...]
    t_exp = jnp.where(keep, jnp.exp(t_logits), 0.0)
    s_exp = jnp.where(keep, jnp.exp(s_logits), 0.0)
    t_down = jnp.sum(t_exp, 1, keepdims=True)
    s_down = jnp.sum(s_exp, 1, keepdims=True)
    t_along = jnp.sum(t_exp, 0, keepdims=True)
    s_along = jnp.sum(s_exp, 0, keepdims=True)
    s_log = s_logits - jnp.log(s_down)
    t_log = t_logits - jnp.log(t_down)
    terms = jnp.where(partner, -s_log, 0.0)
    terms = terms + jnp.where(keep, t_exp / t_down * (t_log - s_log), 0.0)
    loss[...] = jnp.sum(jnp.sum(terms, 1, keepdims=True), 0, keepdims=True)
    both = 2.0 * (s_exp / s_down + s_exp / s_along) - (t_exp / t_down + t_exp / t_along)
    both = both - jnp.where(partner, 2.0, 0.0)
    units = unit[...]
    unit_grad = (
        jnp.dot(both, units, precision=highest, preferred_element_type=f32) / student_softness
    )
    along = jnp.sum(units * unit_grad, -1, keepdims=True)
    raw_low = ((unit_grad - units * along) / norms[...]).astype(bf16)
    low[...] = raw_low
    raw[...] = raw_low.astype(f32)
    mine = raw[pl.ds(pl.multiple_of(place[0] * scale.shape[0], scale.shape[0]), scale.shape[0]), :]
    copy.wait()
    pool_grad = lax.dot_general(
        mine.astype(bf16), weights[...], (((1,), (1,)), ((), ())), preferred_element_type=f32
    )
    for doc in range(scale.shape[0]):
        scale[doc : doc + 1, :] = pool_grad[doc : doc + 1, :] / lens[doc].astype(f32)
    weigh_fetched(copies, scale, held, outs)


def contrast(place, lengths, gram_kept, gram_arrived, logits, unit, norms, w_out, grads, orders, members):
    total_docs, width = unit.shape
    local_docs, hidden = lengths.shape[0], w_out.shape[0]
    buffers, arrived, sums = block_shapes(grads, members)
    vmem, smem = pl.BlockSpec(memory_space=pltpu.VMEM), pl.BlockSpec(memory_space=pltpu.SMEM)
    hbm = pl.BlockSpec(memory_space=pltpu.HBM)
    return pl.pallas_call(
        functools.partial(contrast_kernel, (orders, members // 2)),
        in_specs=[smem] * 2 + [vmem] * 5 + [hbm] * (1 + len(grads)),
        out_specs=[vmem] * 5,
        out_shape=[
            jax.ShapeDtypeStruct((1, 1), f32),
            jax.ShapeDtypeStruct((total_docs, width), bf16),
            jax.ShapeDtypeStruct((local_docs, hidden), f32),
        ]
        + sums,
        scratch_shapes=[pltpu.VMEM((total_docs, width), f32), pltpu.VMEM(w_out.shape, bf16)]
        + buffers
        + [pltpu.SemaphoreType.DMA, arrived],
        compiler_params=pltpu.CompilerParams(vmem_limit_bytes=50 << 20),
        name="contrast",
    )(place, lengths, gram_kept, gram_arrived, logits, unit, norms, w_out, *grads)


def weigh_kernel(plan, parts, place, scale, *refs):
    grads, outs, held, arrived = refs[:parts], refs[-3 - parts : -1 - parts], refs[-1 - parts : -1], refs[-1]
    weigh_fetched(fetch(plan, place, grads, held, arrived), scale, held, outs)


def weigh(place, scale, grads, orders, members, after):
    buffers, arrived, sums = block_shapes(grads, members)
    vmem, smem = pl.BlockSpec(memory_space=pltpu.VMEM), pl.BlockSpec(memory_space=pltpu.SMEM)
    hbm, kept = pl.BlockSpec(memory_space=pltpu.HBM), pl.BlockSpec(memory_space=pl.ANY)
    return pl.pallas_call(
        functools.partial(weigh_kernel, (orders, 0), len(grads)),
        in_specs=[smem, vmem] + [hbm] * len(grads) + [kept] * len(after),
        out_specs=[vmem] * 2,
        out_shape=sums,
        scratch_shapes=buffers + [arrived],
        compiler_params=pltpu.CompilerParams(vmem_limit_bytes=50 << 20),
        name="weigh",
    )(place, scale, *grads, *after)


def finish_kernel(*refs):
    out = refs[-1]
    half = out.shape[1] // 2
    for side in range(2):
        kept, arrived = refs[2 * side : 2 * side + 2]
        out[:, side * half : (side + 1) * half] = kept[0].astype(f32) + arrived[0].astype(f32)


def finish(sides):
    _, rows, half = sides[0][0].shape
    return pl.pallas_call(
        finish_kernel,
        out_shape=jax.ShapeDtypeStruct((rows, 2 * half), f32),
        compiler_params=pltpu.CompilerParams(vmem_limit_bytes=8 << 20),
        name="finish",
    )(*sides[0], *sides[1])


def halving(sent, kept, order, axis):
    for bit in order:
        arrived = swap(sent, axis, bit)
        rest = kept.shape[0] // 2
        if rest:
            sent = (kept[rest:].astype(f32) + arrived[rest:].astype(f32)).astype(bf16)
            kept = (kept[:rest].astype(f32) + arrived[:rest].astype(f32)).astype(bf16)
    return kept, arrived


def on_device(
    student_states,
    lengths,
    student_ln_gain,
    student_w_in,
    student_w_out,
    teacher_rows,
    teacher_mlp_gain,
    teacher_gate_up,
    teacher_down,
    teacher_final_gain,
):
    dp_count = lax.axis_size("dp")
    section_count = lax.axis_size("section")
    dp_index = lax.axis_index("dp")
    section_index = lax.axis_index("section")
    local_docs = teacher_rows.shape[0]
    total_docs = local_docs * dp_count
    col_width = teacher_gate_up.shape[1]
    hidden_width = teacher_gate_up.shape[2]
    place = dp_index.astype(jnp.int32).reshape(1)
    block = hidden_width // 6 if hidden_width % 768 == 0 else hidden_width
    student = functools.partial(
        student_part, lengths, student_states, student_ln_gain, student_w_in
    )
    early = local_docs // 4

    blocks = teacher_rows.reshape(local_docs, dp_count, col_width).transpose(1, 0, 2)
    columns = exchange(blocks, "dp").reshape(total_docs, col_width)
    first = student(teacher_rows, 0, early)
    parts = gate_up(place, columns, teacher_mlp_gain, teacher_gate_up, block)
    parts = parts.reshape(dp_count, local_docs, 2 * hidden_width)
    second = student(parts, early, local_docs - early)
    parts = exchange(parts, "dp")
    hidden = hidden_units(parts, teacher_rows, block)
    every_hidden = exchange(hidden, "dp").reshape(total_docs, hidden_width)
    out = down(every_hidden, teacher_down)
    for bit in range(section_count.bit_length() - 1):
        kept = out if bit == 0 else out.astype(bf16)
        arrived = swap(kept, "section", bit)
        out = kept.astype(f32) + arrived.astype(f32)
    states_block, gram_sum = teacher_block(place, kept, arrived, columns, teacher_final_gain)
    bits = dp_count.bit_length() - 1
    for bit in range(bits):
        gram_kept = gram_sum
        gram_arrived = swap(gram_sum, "dp", bit)
        gram_sum = gram_kept + gram_arrived

    grads, acts, states = zip(first, second)
    pooled_act = jnp.concatenate(acts)[:, 0].astype(bf16)
    pooled_x = jnp.concatenate(states)[:, 0]
    emb_sum = jnp.dot(pooled_act, student_w_out, preferred_element_type=f32)
    for bit in range(section_count.bit_length() - 1):
        emb_sum = emb_sum + swap(emb_sum, "section", bit)
    far_first = tuple(reversed(range(bits)))
    every_raw = (pooled_x + emb_sum)[None]
    for bit in far_first:
        every_raw = jnp.concatenate([every_raw, swap(every_raw, "dp", bit)])
    unit, norms, student_logits = embed(place, every_raw, far_first)
    orders = (tuple(range(bits)), (1, 0) + tuple(range(2, bits)))
    loss, every_low, scale, *sent = contrast(
        place,
        lengths,
        gram_kept,
        gram_arrived,
        student_logits,
        unit,
        norms,
        student_w_out,
        grads,
        orders,
        dp_count,
    )

    kept = weigh(place, scale, grads, orders, dp_count, sent)
    sides = []
    for side in range(2):
        sides.append(halving(sent[side], kept[side], orders[side], "dp"))
    grad_w_in = finish(sides)
    pooled = pooled_act.reshape(local_docs, dp_count, -1).transpose(1, 0, 2).astype(f32)
    states_block = states_block.reshape(dp_count, local_docs, col_width)
    last = exchange(jnp.concatenate([states_block, pooled], axis=2), "dp")
    per_section = dp_count // section_count
    own_blocks = lax.dynamic_slice_in_dim(last, section_index * per_section, per_section, 0)
    own_blocks = own_blocks[:, :, :col_width].transpose(1, 0, 2)
    teacher_states = own_blocks.reshape(local_docs, per_section * col_width)
    pooled_columns = last[:, :, col_width:].reshape(total_docs, -1).astype(bf16)
    grad_w_out = lax.dot_general(
        pooled_columns, every_low, (((0,), (0,)), ((), ())), preferred_element_type=f32
    )
    return (loss[0, 0], grad_w_in, grad_w_out, teacher_states)


def solution(mesh):
    placed = (
        P("dp", None, None),
        P("dp"),
        P(),
        P(None, "section"),
        P("section", None),
        P("dp", None),
        P(),
        P(None, "dp", "section"),
        P("section", "dp"),
        P(),
    )

    return jax.shard_map(
        on_device,
        mesh=mesh,
        in_specs=placed,
        out_specs=(P(), P("dp", "section"), P(("section", "dp"), None), P("dp", "section")),
        check_vma=False,
    )
```
